128 devices in a mesh: ccy: 4 (over z_lo, core), path: 32 (over y, x, z_hi).
Axes of the slice: x: 4, y: 4, z: 4 (z_hi: 2, z_lo: 2; z = z_hi * 2 + z_lo), core: 2. Of those that a mesh axis runs over, the one named last changes fastest.
Arguments:
- curve_store: bfloat16 [4, 64, 64, 8192], P('ccy', 'path'), may hold values from -0.13 to 0.18
- cash_index: int32 [4, 2048, 16], P('ccy'), may hold values from 0 to 1023
- cash_amount: float32 [4, 2048, 16], P('ccy'), may hold values from -0.6 to 0.6
- trade_set: int32 [4, 2048], P('ccy'), may hold values from 0 to 511
- date_slot: int32 [16], replicated, may hold values from 0 to 63, as said below
- default_weight: float32 [16, 512], replicated, may hold values from 0.02 to 0.2
Outputs:
- exposure: float32 [16, 512], P(None, 'ccy')
- node_sens: float32 [4, 16, 64], P('ccy')
The draws below stay inside these ranges and needn't reach their ends.
Inputs may be any that keep to these rules, and one draw needn't show every extreme that they name: `date_slot`: the 16 slots are distinct; slot s is stored at path index s // 2, position s % 2.
All inputs are finite; a program needn't handle non-finite values.
Results may differ from the reference program's by a relative error of at most 0.0029.
Values may be sent and summed in bfloat16 or wider, within the bound.
A program may use at most 64 MiB of HBM per device.

```python
import math
import jax
import jax.numpy as jnp
from jax import lax

NODES = 64
CFG = 1024
NSETS = 512
TRADES = 2048
NCF = 16
DATES = 16
PATHS = 8192
SLOTS_ALL = 64
N_CCY = 4


def draw_date_slot(key, part):
    return jax.random.permutation(key, SLOTS_ALL)[:DATES].astype(jnp.int32)


def draw_curve_store(key, part):
    level_key, spread_key, height_key, flip_key = jax.random.split(jax.random.fold_in(key, 7), 4)
    block_shape = (N_CCY, SLOTS_ALL, 1, PATHS)
    base_level = jax.random.uniform(level_key, block_shape, jnp.float32, 0.0, 0.05)
    jump_scale = jnp.exp(jax.random.uniform(spread_key, block_shape, jnp.float32, math.log(0.01), math.log(0.12)))
    jump_height = jax.random.uniform(height_key, (N_CCY, SLOTS_ALL, NODES, PATHS), jnp.float32, 0.5, 1.0)
    flip_bits = jax.random.randint(flip_key, block_shape, 0, 2)
    node_index = jnp.arange(NODES, dtype=jnp.int32).reshape(1, 1, NODES, 1)
    parity = (node_index + flip_bits) % 2
    signed = 1.0 - 2.0 * parity.astype(jnp.float32)
    return (base_level + jump_scale * signed * jump_height).astype(jnp.bfloat16)


def touch_ends(drawn, key, least, largest):
    spot = [jax.random.randint(jax.random.fold_in(key, axis), (), 0, length) for axis, length in enumerate(drawn.shape)]
    main_axis = drawn.shape.index(max(drawn.shape))
    neighbour = spot[:main_axis] + [(spot[main_axis] + 1) % drawn.shape[main_axis]] + spot[main_axis + 1:]
    return drawn.at[tuple(spot)].set(least).at[tuple(neighbour)].set(largest)


def level_of(own_key, dims, shards, least, top_value):
    def one(dim, blocks):
        draws = jax.random.uniform(jax.random.fold_in(jax.random.fold_in(own_key, 6), dim), (blocks,), jnp.float32, least / len(shards), top_value / len(shards))
        return jnp.repeat(jnp.exp(draws), dims[dim] // blocks).reshape((-1,) + (1,) * (len(dims) - dim - 1))

    gain = one(*shards[0])
    for cut in shards[1:]:
        gain = gain * one(*cut)
    return gain


def noise(stream_key, extent, scale, most, shards=(), held_as=jnp.bfloat16):
    entries = jax.random.normal(stream_key, extent, jnp.float32) * scale
    if len(shards) > 0:
        entries = level_of(stream_key, extent, shards, -0.22, 0.18) * entries
    return jnp.clip(entries, min=-most, max=most).astype(held_as)


def setup_inputs(seed: int = 0) -> dict:
    key_list = jax.random.split(jax.random.key(seed), 7)
    return {
        "curve_store": draw_curve_store(jax.random.fold_in(key_list[6], 71), 0),
        "cash_index": touch_ends(jax.random.randint(key_list[1], (N_CCY, TRADES, NCF), 0, CFG), jax.random.fold_in(key_list[1], 1), 0, CFG - 1).astype(jnp.int32),
        "cash_amount": noise(key_list[2], (N_CCY, TRADES, NCF), 0.1, 0.6, ((0, 4),), jnp.float32),
        "trade_set": touch_ends(jax.random.randint(key_list[3], (N_CCY, TRADES), 0, NSETS), jax.random.fold_in(key_list[3], 1), 0, NSETS - 1).astype(jnp.int32),
        "date_slot": draw_date_slot(jax.random.fold_in(key_list[6], 71), 0),
        "default_weight": jnp.clip(jnp.exp(jax.random.uniform(key_list[5], (DATES, NSETS), jnp.float32, math.log(0.02), math.log(0.2))), 0.02, 0.2),
    }


SOFTEN = 0.04
HORIZON = 32.0

def date_tables(date_index, node_count, grid_count):
    start_time = 0.5 * (jnp.asarray(date_index).astype(jnp.float32) + 1.0)
    grid_times = HORIZON * (jnp.arange(grid_count, dtype=jnp.float32) + 1.0) / grid_count
    tenors = HORIZON * (jnp.arange(node_count, dtype=jnp.float32) + 1.0) / node_count
    remain = grid_times - start_time
    alive_mask = (remain > 0.0).astype(jnp.float32)
    clipped = jnp.clip(remain, HORIZON / node_count, HORIZON)
    weights = jnp.maximum(0.0, 1.0 - jnp.abs(clipped[None, :] - tenors[:, None]) * (node_count / HORIZON))
    return (remain, alive_mask, weights)

def netted_cash(flow_index, amount, trade_sets):
    columns = jnp.repeat(trade_sets, flow_index.shape[1]).astype(jnp.int32)
    cash_table = jnp.zeros((CFG, NSETS), jnp.float32).at[flow_index.reshape(-1).astype(jnp.int32), columns].add(amount.reshape(-1).astype(jnp.float32))
    return cash_table.astype(jnp.bfloat16)

def reference(curve_store, cash_index, cash_amount, trade_set, date_slot, default_weight):
    total_paths = curve_store.shape[3]
    tables = [netted_cash(cash_index[member], cash_amount[member], trade_set[member]) for member in range(N_CCY)]
    exposure_rows = []
    sens_rows = []
    for date_index in range(DATES):
        remain, alive_mask, weights = date_tables(date_index, NODES, CFG)
        grid_weights = weights.astype(jnp.bfloat16)
        values = jnp.zeros((total_paths, NSETS), jnp.float32)
        discounts = []
        for member in range(N_CCY):
            curve_now = lax.dynamic_index_in_dim(curve_store[member], date_slot[date_index].astype(jnp.int32), 0, keepdims=False)
            yields = lax.dot_general(curve_now, grid_weights, (((0,), (0,)), ((), ())), preferred_element_type=jnp.float32)
            discount = alive_mask * jnp.exp(-yields * remain)
            discounts.append(discount)
            values = values + jnp.dot(discount.astype(jnp.bfloat16), tables[member], preferred_element_type=jnp.float32)
        rooted = jnp.sqrt(values * values + SOFTEN)
        exposure_rows.append(lax.optimization_barrier(jnp.sum(0.5 * (values + rooted), axis=0)) / total_paths)
        slopes = (default_weight[date_index] / total_paths * 0.5 * (1.0 + values / rooted)).astype(jnp.bfloat16)
        group_sens = []
        for member in range(N_CCY):
            back_flow = lax.dot_general(slopes, tables[member], (((1,), (1,)), ((), ())), preferred_element_type=jnp.float32)
            node_pull = lax.optimization_barrier(jnp.sum(back_flow * -remain * discounts[member], axis=0))
            group_sens.append(jnp.dot(weights, node_pull, precision=lax.Precision.HIGHEST))
        sens_rows.append(jnp.stack(group_sens))
    return (jnp.stack(exposure_rows), jnp.stack(sens_rows, axis=1))
```

```python
import functools

import jax
import jax.numpy as jnp
from jax import lax
from jax.experimental import pallas as pl
from jax.experimental.pallas import tpu as pltpu
from jax.sharding import PartitionSpec as P

NODES = 64
CFG = 1024
NSETS = 512
NCF = 16
TRADES = 2048
DATES = 16
HALF = DATES // 2
CHIP_PATHS = 128
TOTAL_PATHS = 8192
SOFTEN = 0.04
CHUNK = 256
CHUNKS = CFG // CHUNK
ROWS = 512
MESH = pl.DeviceIdType.MESH
BF = jnp.bfloat16
F32 = jnp.float32
NT = (((1,), (1,)), ((), ()))
TN = (((0,), (0,)), ((), ()))


def coords():
    ccy = lax.axis_index("ccy")
    path = lax.axis_index("path")
    core = lax.rem(ccy, 2)
    z = lax.rem(path, 2) * 2 + lax.div(ccy, 2)
    x = lax.rem(lax.div(path, 2), 4)
    y = lax.div(path, 8)
    return y, x, z, core


def device(y, x, z, core):
    return (lax.rem(z, 2) * 2 + core, (y * 4 + x) * 2 + lax.div(z, 2))


def chip_index(y, x, z):
    return (y * 4 + x) * 4 + z


def shifted(i, y, x, z):
    b, c, a = lax.div(i, 16), lax.rem(lax.div(i, 4), 4), lax.rem(i, 4)
    return (
        lax.rem(y + a, 4),
        lax.rem(x + a + b, 4),
        lax.rem(z + a + c, 4),
    )


def remote(src, dst, send, recv, target):
    return pltpu.make_async_remote_copy(
        src_ref=src,
        dst_ref=dst,
        send_sem=send,
        recv_sem=recv,
        device_id=target,
        device_id_type=MESH,
    )


def exchange_kernel(
    slot_ref, store, idx_ref, amt_ref, set_ref,
    tables, curves,
    got, keep, give, bidx, bhi, blo, onehot, flows, made,
    a_send, a_recv, own_sem, p_send, p_recv, l_sem, z_send, z_recv, f_send, f_recv,
    c_send, c_recv,
):
    y, x, z, core = coords()
    group = lax.rem(z, 2) * 2 + core
    partner = device(y, x, z, 1 - core)
    up = device(y, x, lax.rem(z + 1, 4), core)
    down = device(y, x, lax.rem(z + 3, 4), core)
    me = chip_index(y, x, z)

    barrier = pltpu.get_barrier_semaphore()

    def greet(i, carry):
        pl.semaphore_signal(
            barrier, inc=1, device_id=device(*shifted(i, y, x, z), core), device_id_type=MESH
        )
        return carry

    pl.semaphore_signal(barrier, inc=1, device_id=partner, device_id_type=MESH)
    lax.fori_loop(1, 64, greet, 0)
    pl.semaphore_wait(barrier, 64)

    def lanes(chip):
        return pl.ds(pl.multiple_of(chip * CHIP_PATHS, CHIP_PATHS), CHIP_PATHS)

    def curve_copy(i):
        ty, tx, tz = shifted(i, y, x, z)
        return remote(
            store.at[0, :, :, lanes(chip_index(ty, tx, tz))],
            got.at[me],
            a_send.at[i],
            a_recv.at[me],
            device(ty, tx, tz, core),
        )

    def launch(i, carry):
        curve_copy(i).start()
        return carry

    lax.fori_loop(1, 64, launch, 0)
    own_copy = pltpu.make_async_copy(store.at[0, :, :, lanes(me)], got.at[me], own_sem)
    own_copy.start()

    amounts = amt_ref[...]
    indices = idx_ref[...]
    merged = jnp.zeros_like(amounts)
    for k in range(NCF):
        merged = merged + jnp.where(indices == indices[k : k + 1], amounts[k : k + 1], 0.0)
    high = merged.astype(BF).astype(F32)
    low = merged - high
    for k in range(NCF):
        bhi[k] = jnp.broadcast_to(high[k : k + 1], (16, TRADES)).astype(BF)
        blo[k] = jnp.broadcast_to(low[k : k + 1], (16, TRADES)).astype(BF)
    sets = set_ref[...]
    for s in range(0, NSETS, 64):
        ids = lax.broadcasted_iota(jnp.int32, (64, TRADES), 0) + s
        onehot[pl.ds(s, 64), :] = jnp.where(ids == sets, 1.0, 0.0).astype(BF)

    def make_chunk(q, carry):
        base = q * CHUNK
        for k in range(NCF):
            near = jnp.clip(idx_ref[pl.ds(k, 1), :] - base, -1, CHUNK).astype(F32)
            bidx[k] = jnp.broadcast_to(near, (16, TRADES)).astype(BF)

        def spread(t, inner):
            cols = pl.ds(pl.multiple_of(t * 256, 256), 256)
            for sub in range(4):
                ids = (
                    lax.broadcasted_iota(jnp.int32, (4, 16, 256), 0) * 16
                    + lax.broadcasted_iota(jnp.int32, (4, 16, 256), 1)
                    + sub * 64
                ).astype(F32).astype(BF)
                acc_hi = jnp.zeros((4, 16, 256), BF)
                acc_lo = jnp.zeros((4, 16, 256), BF)
                for k in range(NCF):
                    hit = ids == bidx[k, :, cols][None]
                    acc_hi = jnp.where(hit, bhi[k, :, cols][None], acc_hi)
                    acc_lo = jnp.where(hit, blo[k, :, cols][None], acc_lo)
                flows[pl.ds(sub * 64, 64), cols] = acc_hi.reshape(64, 256)
                flows[pl.ds(CHUNK + sub * 64, 64), cols] = acc_lo.reshape(64, 256)
            return inner

        lax.fori_loop(0, TRADES // 256, spread, 0)
        both = lax.dot_general(flows[...], onehot[...], NT, preferred_element_type=F32)
        made[q] = (both[:CHUNK] + both[CHUNK:]).astype(BF)
        return carry

    lax.fori_loop(0, CHUNKS, make_chunk, 0)

    def rows(q):
        return pl.ds(pl.multiple_of(q * CHUNK, CHUNK), CHUNK)

    local = [
        pltpu.make_async_copy(made.at[q], tables.at[group, rows(q), :], l_sem.at[q])
        for q in range(CHUNKS)
    ]
    across = [
        remote(made.at[q], tables.at[group, rows(q), :], z_send.at[q], z_recv.at[q], up if q < 2 else down)
        for q in range(CHUNKS)
    ]
    beside = [
        remote(made.at[q], tables.at[group, rows(q), :], p_send.at[q], p_recv.at[q], partner)
        for q in range(CHUNKS)
    ]
    for q in range(CHUNKS):
        across[q].start()
        beside[q].start()
        local[q].start()

    other = lax.rem(group + 2, 4)
    arriving = [
        remote(made.at[q], tables.at[other, rows(q), :], z_send.at[q], z_recv.at[q], up if q < 2 else down)
        for q in range(CHUNKS)
    ]
    forward = [
        remote(tables.at[other, rows(q), :], tables.at[other, rows(q), :], f_send.at[q], f_recv.at[q], partner)
        for q in range(CHUNKS)
    ]
    for q in (0, 2, 1, 3):
        arriving[q].wait_recv()
        forward[q].start()

    def landed(i, carry):
        curve_copy(i).wait_send()
        ty, tx, tz = shifted(i, y, x, z)
        source = chip_index(ty, tx, tz)
        remote(
            store.at[0, :, :, lanes(me)], got.at[source], a_send.at[i], a_recv.at[source],
            device(ty, tx, tz, core),
        ).wait_recv()
        return carry

    own_copy.wait()
    lax.fori_loop(1, 64, landed, 0)

    def pick(date, low_z):
        slot = slot_ref[date]
        place = lax.div(slot, 2)
        return got[lax.div(place, 2) * 4 + lax.rem(place, 2) * 2 + low_z, lax.rem(slot, 2)]

    for k in range(HALF):
        for low_z in range(2):
            give[low_z, k] = pick((1 - core) * HALF + k, low_z)
            keep[low_z, k] = pick(core * HALF + k, low_z)
    trade = remote(give, curves.at[core], c_send, c_recv, partner)
    trade.start()
    own = pltpu.make_async_copy(keep, curves.at[core], own_sem)
    own.start()
    own.wait()
    trade.wait_send()
    remote(give, curves.at[1 - core], c_send, c_recv, partner).wait_recv()
    for q in range(CHUNKS):
        local[q].wait()
        across[q].wait_send()
        beside[q].wait_send()
        remote(
            made.at[q], tables.at[lax.rem(z, 2) * 2 + 1 - core, rows(q), :], p_send.at[q], p_recv.at[q], partner
        ).wait_recv()
        forward[q].wait_send()
        remote(
            made.at[q], tables.at[lax.rem(z + 1, 2) * 2 + 1 - core, rows(q), :], f_send.at[q], f_recv.at[q], partner
        ).wait_recv()


def exchange(date_slot, curve_store, indices, amounts, sets):
    whole = pl.BlockSpec(memory_space=pltpu.VMEM)
    dma = pltpu.SemaphoreType.DMA
    return pl.pallas_call(
        exchange_kernel,
        out_shape=(
            jax.ShapeDtypeStruct((4, CFG, NSETS), BF),
            jax.ShapeDtypeStruct((2, 2, HALF, NODES, CHIP_PATHS), BF),
        ),
        in_specs=[
            pl.BlockSpec(memory_space=pltpu.SMEM),
            pl.BlockSpec(memory_space=pl.ANY),
            whole,
            whole,
            whole,
        ],
        out_specs=(pl.BlockSpec(memory_space=pl.ANY), pl.BlockSpec(memory_space=pl.ANY)),
        scratch_shapes=[
            pltpu.VMEM((64, 2, NODES, CHIP_PATHS), BF),
            pltpu.VMEM((2, HALF, NODES, CHIP_PATHS), BF),
            pltpu.VMEM((2, HALF, NODES, CHIP_PATHS), BF),
            pltpu.VMEM((NCF, 16, TRADES), BF),
            pltpu.VMEM((NCF, 16, TRADES), BF),
            pltpu.VMEM((NCF, 16, TRADES), BF),
            pltpu.VMEM((NSETS, TRADES), BF),
            pltpu.VMEM((2 * CHUNK, TRADES), BF),
            pltpu.VMEM((CHUNKS, CHUNK, NSETS), BF),
            dma((64,)),
            dma((64,)),
            dma,
            dma((CHUNKS,)),
            dma((CHUNKS,)),
            dma((CHUNKS,)),
            dma((CHUNKS,)),
            dma((CHUNKS,)),
            dma((CHUNKS,)),
            dma((CHUNKS,)),
            dma,
            dma,
        ],
        compiler_params=pltpu.CompilerParams(
            collective_id=0, has_side_effects=True, vmem_limit_bytes=56 * 1024 * 1024
        ),
    )(date_slot, curve_store, indices, amounts, sets)


def grid_tables(date, nodes):
    steps = lax.broadcasted_iota(jnp.int32, (1, CFG), 1) + 1 - 16 * (date + 1)
    steps = steps.astype(F32)
    place = jnp.clip(steps * (1.0 / 16.0), 1.0, float(NODES))
    node = (lax.broadcasted_iota(jnp.int32, (nodes, CFG), 0) + 1).astype(F32)
    weights = jnp.maximum(0.0, 1.0 - jnp.abs(place - node))
    return steps, steps * (1.0 / 32.0), weights


def price_kernel(core_ref, tables, curves, weight_ref, out, discount, value, slope, pull):
    core = core_ref[0]

    def discounts(k, carry):
        steps, remain, weights = grid_tables(core * HALF + k, NODES)
        weights = weights.astype(BF)
        down = remain * -1.0
        live = steps > 0.0
        for g in range(4):
            block = curves[g % 2, g // 2, k]
            rate = lax.dot_general(block, weights, TN, preferred_element_type=F32)
            held = jnp.where(live, jnp.exp(rate * down), 0.0)
            discount[pl.ds(pl.multiple_of(k * CHIP_PATHS, CHIP_PATHS), CHIP_PATHS), pl.ds(g * CFG, CFG)] = (
                held.astype(BF)
            )
        return carry

    lax.fori_loop(0, HALF, discounts, 0)

    per_block = ROWS // CHIP_PATHS

    def block(b, carry):
        span = pl.ds(pl.multiple_of(b * ROWS, ROWS), ROWS)
        value[...] = jnp.zeros_like(value)

        def add_group(g, inner):
            cols = pl.ds(pl.multiple_of(g * CFG, CFG), CFG)
            value[...] += jnp.dot(discount[span, cols], tables[g], preferred_element_type=F32)
            return inner

        lax.fori_loop(0, 4, add_group, 0)
        for i in range(per_block):
            k = b * per_block + i
            v = value[pl.ds(i * CHIP_PATHS, CHIP_PATHS), :]
            square = v * v + SOFTEN
            inverse = lax.rsqrt(square)
            mean = jnp.sum(0.5 * (v + square * inverse), axis=0, keepdims=True) * (1.0 / TOTAL_PATHS)
            scale = weight_ref[pl.ds(k, 1), :] * (0.5 / TOTAL_PATHS)
            slope[pl.ds(i * CHIP_PATHS, CHIP_PATHS), :] = (scale * (1.0 + v * inverse)).astype(BF)
            for part in range(4):
                out[part // 2, part % 2, pl.ds(k, 1), :] = mean[:, part * 128 : (part + 1) * 128]

        def pull_group(n, inner):
            g, c = lax.div(n, CHUNKS), lax.rem(n, CHUNKS)
            cash = tables[g, pl.ds(pl.multiple_of(c * CHUNK, CHUNK), CHUNK), :]
            back = lax.dot_general(slope[...], cash, NT, preferred_element_type=F32)
            cols = pl.ds(pl.multiple_of(n * CHUNK, CHUNK), CHUNK)
            weighed = back * discount[span, cols].astype(F32)
            sums = weighed.reshape(per_block, CHIP_PATHS, CHUNK).sum(axis=1)
            for i in range(per_block):
                pull[b * per_block + i, pl.ds(g, 1), pl.ds(pl.multiple_of(c * CHUNK, CHUNK), CHUNK)] = sums[i : i + 1]
            return inner

        lax.fori_loop(0, 4 * CHUNKS, pull_group, 0)
        return carry

    lax.fori_loop(0, HALF // per_block, block, 0)

    def sensitivities(k, carry):
        _, remain, weights = grid_tables(core * HALF + k, 128)
        weights = weights.astype(BF)
        rest = pull[k] * (remain * -1.0)
        total = jnp.zeros((4, 128), F32)
        for _ in range(3):
            part = rest.astype(BF)
            total = total + lax.dot_general(part, weights, NT, preferred_element_type=F32)
            rest = rest - part.astype(F32)
        for g in range(4):
            out[g // 2, g % 2, pl.ds(HALF + k, 1), :] = total[g : g + 1]
        return carry

    lax.fori_loop(0, HALF, sensitivities, 0)


def price(core, tables, curves, weights):
    whole = pl.BlockSpec(memory_space=pltpu.VMEM)
    paths = HALF * CHIP_PATHS
    return pl.pallas_call(
        price_kernel,
        out_shape=jax.ShapeDtypeStruct((2, 2, 2 * HALF, 128), F32),
        in_specs=[pl.BlockSpec(memory_space=pltpu.SMEM), whole, whole, whole],
        out_specs=whole,
        scratch_shapes=[
            pltpu.VMEM((paths, 4 * CFG), BF),
            pltpu.VMEM((ROWS, NSETS), F32),
            pltpu.VMEM((ROWS, NSETS), BF),
            pltpu.VMEM((HALF, 4, CFG), F32),
        ],
        compiler_params=pltpu.CompilerParams(vmem_limit_bytes=56 * 1024 * 1024),
    )(core, tables, curves, weights)


def total_kernel(
    part, expo, sens, z_buf, y_buf, x_buf, c_buf,
    z_send, z_recv, y_send, y_recv, x_send, x_recv, c_send, c_recv,
):
    y, x, z, core = coords()
    low = lax.rem(z, 2)
    partner = device(y, x, z, 1 - core)
    in_z = [(z + i) % 4 for i in range(1, 4)]
    in_y = [(y + i) % 4 for i in range(1, 4)]
    in_x = [(x + i) % 4 for i in range(1, 4)]
    barrier = pltpu.get_barrier_semaphore()
    targets = (
        [device(y, x, t, core) for t in in_z]
        + [device(t, x, z, core) for t in in_y]
        + [device(y, t, z, core) for t in in_x]
        + [partner]
    )
    for t in targets:
        pl.semaphore_signal(barrier, inc=1, device_id=t, device_id_type=MESH)
    pl.semaphore_wait(barrier, len(targets))

    def stage(source_of, buf, send, recv, here, others, device_of):
        sends = []
        for i, t in enumerate(others):
            copy = remote(source_of(t), buf.at[here], send.at[i], recv.at[here], device_of(t))
            copy.start()
            sends.append(copy)
        for i, t in enumerate(others):
            sends[i].wait_send()
            remote(source_of(here), buf.at[t], send.at[i], recv.at[t], device_of(t)).wait_recv()

    z_buf[z] = part[low]
    stage(
        lambda t: part.at[lax.rem(t, 2)], z_buf, z_send, z_recv, z, in_z,
        lambda t: device(y, x, t, core),
    )
    y_buf[y] = (z_buf[0] + z_buf[1]) + (z_buf[2] + z_buf[3])
    stage(lambda t: y_buf.at[y], y_buf, y_send, y_recv, y, in_y, lambda t: device(t, x, z, core))
    x_buf[x] = (y_buf[0] + y_buf[1]) + (y_buf[2] + y_buf[3])
    stage(lambda t: x_buf.at[x], x_buf, x_send, x_recv, x, in_x, lambda t: device(y, t, z, core))
    c_buf[core] = (x_buf[0] + x_buf[1]) + (x_buf[2] + x_buf[3])
    trade = remote(c_buf.at[core, 1 - core], c_buf.at[core, 1 - core], c_send, c_recv, partner)
    trade.start()
    trade.wait_send()
    remote(c_buf.at[core, core], c_buf.at[1 - core, core], c_send, c_recv, partner).wait_recv()
    for half in range(2):
        block = c_buf[half, core]
        expo[pl.ds(half * HALF, HALF), :] = block[:HALF]
        sens[0, pl.ds(half * HALF, HALF), :] = block[HALF:, :NODES]


def total(part):
    whole = pl.BlockSpec(memory_space=pltpu.VMEM)
    dma = pltpu.SemaphoreType.DMA
    half = (2, 2 * HALF, 128)
    return pl.pallas_call(
        total_kernel,
        out_shape=(
            jax.ShapeDtypeStruct((DATES, NSETS // 4), F32),
            jax.ShapeDtypeStruct((1, DATES, NODES), F32),
        ),
        in_specs=[whole],
        out_specs=(whole, whole),
        scratch_shapes=[
            pltpu.VMEM((4, *half), F32),
            pltpu.VMEM((4, *half), F32),
            pltpu.VMEM((4, *half), F32),
            pltpu.VMEM((2, *half), F32),
            dma((3,)),
            dma((4,)),
            dma((3,)),
            dma((4,)),
            dma((3,)),
            dma((4,)),
            dma,
            dma,
        ],
        compiler_params=pltpu.CompilerParams(collective_id=1, has_side_effects=True),
    )(part)


def local(curve_store, cash_index, cash_amount, trade_set, date_slot, default_weight):
    core = lax.rem(lax.axis_index("ccy"), 2)
    tables, curves = exchange(
        date_slot, curve_store, cash_index[0].T, cash_amount[0].T, trade_set
    )
    weights = lax.dynamic_slice_in_dim(default_weight, core * HALF, HALF, 0)
    part = price(core.reshape(1), tables, curves, weights)
    return total(part)


def solution(mesh):
    in_specs = (
        P("ccy", "path", None, None),
        P("ccy", None, None),
        P("ccy", None, None),
        P("ccy", None),
        P(),
        P(),
    )
    out_specs = (P(None, "ccy"), P("ccy", None, None))
    return jax.shard_map(local, mesh=mesh, in_specs=in_specs, out_specs=out_specs, check_vma=False)
```

```python
import jax
import jax.numpy as jnp
from jax import lax
from jax.experimental import pallas as pl
from jax.experimental.pallas import tpu as pltpu
from jax.sharding import PartitionSpec as P

NODES = 64
CFG = 1024
NSETS = 512
NCF = 16
TRADES = 2048
DATES = 16
HALF = DATES // 2
CHIP_PATHS = 128
ROWS = HALF * CHIP_PATHS
TOTAL_PATHS = 8192
SOFTEN = 0.04
LOG2E = 1.4426950408889634
CHUNK = 256
CHUNKS = CFG // CHUNK
TAPS = 24
MESH = pl.DeviceIdType.MESH
BF = jnp.bfloat16
F32 = jnp.float32
NT = (((1,), (1,)), ((), ()))
TN = (((0,), (0,)), ((), ()))


def coords():
    ccy = lax.axis_index("ccy")
    path = lax.axis_index("path")
    core = lax.rem(ccy, 2)
    z = lax.rem(path, 2) * 2 + lax.div(ccy, 2)
    x = lax.rem(lax.div(path, 2), 4)
    y = lax.div(path, 8)
    return y, x, z, core


def device(y, x, z, core):
    return (lax.rem(z, 2) * 2 + core, (y * 4 + x) * 2 + lax.div(z, 2))


def chip_index(y, x, z):
    return (y * 4 + x) * 4 + z


def shifted(i, y, x, z):
    b, c, a = lax.div(i, 16), lax.rem(lax.div(i, 4), 4), lax.rem(i, 4)
    return (
        lax.rem(y + a, 4),
        lax.rem(x + a + b, 4),
        lax.rem(z + a + c, 4),
    )


def remote(src, dst, send, recv, target):
    return pltpu.make_async_remote_copy(
        src_ref=src,
        dst_ref=dst,
        send_sem=send,
        recv_sem=recv,
        device_id=target,
        device_id_type=MESH,
    )


def aligned(start, size):
    return pl.ds(pl.multiple_of(start, size), size)


def grid_tables(date, nodes):
    steps = lax.broadcasted_iota(jnp.int32, (1, CFG), 1) + 1 - 16 * (date + 1)
    steps = steps.astype(F32)
    place = jnp.clip(steps * (1.0 / 16.0), 1.0, float(NODES))
    node = (lax.broadcasted_iota(jnp.int32, (nodes, CFG), 0) + 1).astype(F32)
    weights = jnp.maximum(0.0, 1.0 - jnp.abs(place - node))
    return steps, steps * (1.0 / 32.0), weights


def build_table(raw_i, raw_a, j, slot, tables, bidx, bhi, blo, onehot, flows, send_chunk):
    amounts = raw_a[j]
    indices = raw_i[j, pl.ds(0, NCF), :]
    merged = jnp.zeros_like(amounts)
    for k in range(NCF):
        merged = merged + jnp.where(indices == indices[k : k + 1], amounts[k : k + 1], 0.0)
    high = merged.astype(BF).astype(F32)
    low = merged - high
    for k in range(NCF):
        bhi[k] = jnp.broadcast_to(high[k : k + 1], (16, TRADES)).astype(BF)
        blo[k] = jnp.broadcast_to(low[k : k + 1], (16, TRADES)).astype(BF)
    sets = raw_i[j, pl.ds(NCF, 1), :]
    for s in range(0, NSETS, 64):
        ids = lax.broadcasted_iota(jnp.int32, (64, TRADES), 0) + s
        onehot[pl.ds(s, 64), :] = jnp.where(ids == sets, 1.0, 0.0).astype(BF)

    def make_chunk(q, carry):
        base = q * CHUNK
        for k in range(NCF):
            near = jnp.clip(raw_i[j, pl.ds(k, 1), :] - base, -1, CHUNK).astype(F32)
            bidx[k] = jnp.broadcast_to(near, (16, TRADES)).astype(BF)

        def spread(t, inner):
            cols = aligned(t * 128, 128)
            where = [bidx[k, :, cols] for k in range(NCF)]
            tops = [bhi[k, :, cols] for k in range(NCF)]
            lows = [blo[k, :, cols] for k in range(NCF)]
            for sub in range(CHUNK // 32):
                ids = (
                    lax.broadcasted_iota(jnp.int32, (2, 16, 128), 0) * 16
                    + lax.broadcasted_iota(jnp.int32, (2, 16, 128), 1)
                    + sub * 32
                ).astype(F32).astype(BF)
                acc_hi = jnp.zeros((2, 16, 128), BF)
                acc_lo = jnp.zeros((2, 16, 128), BF)
                for k in range(NCF):
                    hit = ids == where[k][None]
                    acc_hi = jnp.where(hit, tops[k][None], acc_hi)
                    acc_lo = jnp.where(hit, lows[k][None], acc_lo)
                flows[pl.ds(sub * 32, 32), cols] = acc_hi.reshape(32, 128)
                flows[pl.ds(CHUNK + sub * 32, 32), cols] = acc_lo.reshape(32, 128)
            return inner

        lax.fori_loop(0, TRADES // 128, spread, 0)
        both = lax.dot_general(flows[...], onehot[...], NT, preferred_element_type=F32)
        tables[slot, aligned(q * CHUNK, CHUNK), :] = (both[:CHUNK] + both[CHUNK:]).astype(BF)
        send_chunk(q)
        return carry

    lax.fori_loop(0, CHUNKS, make_chunk, 0)


def price(core, tables, curves, weight_ref, part, discount, value, slope, pull, mesh_w):
    for k in range(HALF):
        pull[k] = jnp.zeros((8, CFG), F32)
    part[...] = jnp.zeros_like(part)

    def discounts(k, carry):
        steps, remain, weights = grid_tables(core * HALF + k, NODES)
        weights = weights.astype(BF)
        mesh_w[k] = weights
        down = remain * -LOG2E
        live = steps[:, :256] > 0.0
        for g in range(4):
            rate = lax.dot_general(curves[g % 2, g // 2, k], weights, TN, preferred_element_type=F32)
            held = jnp.exp2(rate * down)
            rows = aligned(k * CHIP_PATHS, CHIP_PATHS)
            discount[rows, pl.ds(g * CFG, 256)] = jnp.where(live, held[:, :256], 0.0).astype(BF)
            discount[rows, pl.ds(g * CFG + 256, CFG - 256)] = held[:, 256:].astype(BF)
        return carry

    lax.fori_loop(0, HALF, discounts, 0)

    value[...] = jnp.dot(discount[:, pl.ds(0, CFG)], tables[0], preferred_element_type=F32)

    def add_group(g, carry):
        value[...] += jnp.dot(discount[:, aligned(g * CFG, CFG)], tables[g], preferred_element_type=F32)
        return carry

    lax.fori_loop(1, 4, add_group, 0)

    def slopes(k, carry):
        rows = aligned(k * CHIP_PATHS, CHIP_PATHS)
        v = value[rows, :]
        square = v * v + SOFTEN
        inverse = lax.rsqrt(square)
        mean = jnp.sum(0.5 * (v + square * inverse), axis=0, keepdims=True) * (1.0 / TOTAL_PATHS)
        scale = weight_ref[pl.ds(core * HALF + k, 1), :] * (0.5 / TOTAL_PATHS)
        slope[rows, :] = (scale * (1.0 + v * inverse)).astype(BF)
        for i in range(4):
            part[i // 2, i % 2, pl.ds(k, 1), :] = mean[:, i * 128 : (i + 1) * 128]
        return carry

    lax.fori_loop(0, HALF, slopes, 0)

    def pull_group(n, carry):
        g, c = lax.div(n, CHUNKS), lax.rem(n, CHUNKS)
        cash = tables[g, aligned(c * CHUNK, CHUNK), :]
        back = lax.dot_general(slope[...], cash, NT, preferred_element_type=F32)
        weighed = back * discount[:, aligned(n * CHUNK, CHUNK)].astype(F32)
        sums = weighed.reshape(HALF, CHIP_PATHS, CHUNK).sum(axis=1)
        for k in range(HALF):
            pull[k, pl.ds(g, 1), aligned(c * CHUNK, CHUNK)] = sums[k : k + 1]
        return carry

    lax.fori_loop(0, 4 * CHUNKS, pull_group, 0)

    for k in range(HALF):
        _, remain, _ = grid_tables(core * HALF + k, 8)
        rest = pull[k] * (remain * -1.0)
        pieces = []
        for _ in range(3):
            piece = rest.astype(BF).astype(F32)
            rest = rest - piece
            pieces.append(piece)
        pieces.append(jnp.zeros_like(rest))
        stack = jnp.concatenate(pieces, axis=0).astype(BF)
        sums = lax.dot_general(stack, mesh_w[k], NT, preferred_element_type=F32)
        total = sums[:8] + sums[8:16] + sums[16:24]
        for g in range(4):
            part[g // 2, g % 2, pl.ds(HALF + k, 1), pl.ds(0, NODES)] = total[g : g + 1]


def kernel(
    slot_ref, store, taps, amounts, weight_ref,
    out,
    got, curves, give, raw_i, raw_a, bidx, bhi, blo, onehot, flows, tables,
    discount, value, slope, pull, mesh_w, part, z_buf, y_buf, x_buf,
    a_send, a_recv, own_sem, l_sem, r_send, r_recv, p_send, p_recv, c_send, c_recv,
    z_send, z_recv, y_send, y_recv, x_send, x_recv,
):
    y, x, z, core = coords()
    low = lax.rem(z, 2)
    group = low * 2 + core
    other = (1 - low) * 2 + core
    partner = device(y, x, z, 1 - core)
    up = device(y, x, lax.rem(z + 1, 4), core)
    down = device(y, x, lax.rem(z + 3, 4), core)
    me = chip_index(y, x, z)
    in_z = [lax.rem(z + i, 4) for i in range(1, 4)]
    in_y = [lax.rem(y + i, 4) for i in range(1, 4)]
    in_x = [lax.rem(x + i, 4) for i in range(1, 4)]

    barrier = pltpu.get_barrier_semaphore()

    def greet(i, carry):
        pl.semaphore_signal(
            barrier, inc=1, device_id=device(*shifted(i, y, x, z), core), device_id_type=MESH
        )
        return carry

    pl.semaphore_signal(barrier, inc=1, device_id=partner, device_id_type=MESH)
    for t in in_x:
        pl.semaphore_signal(barrier, inc=1, device_id=device(y, t, z, 1 - core), device_id_type=MESH)
    lax.fori_loop(1, 64, greet, 0)
    own_raw = [
        pltpu.make_async_copy(taps, raw_i.at[0], l_sem.at[0]),
        pltpu.make_async_copy(amounts, raw_a.at[0], l_sem.at[1]),
    ]
    for copy in own_raw:
        copy.start()
    pl.semaphore_wait(barrier, 67)

    halves = [pl.ds(0, TRADES // 2), pl.ds(TRADES // 2, TRADES // 2)]
    raw = []
    for h, target in enumerate((up, down)):
        raw.append(remote(taps.at[:, halves[h]], raw_i.at[1, :, halves[h]], r_send.at[2 * h], r_recv.at[2 * h], target))
        raw.append(
            remote(amounts.at[:, halves[h]], raw_a.at[1, :, halves[h]], r_send.at[2 * h + 1], r_recv.at[2 * h + 1], target)
        )
    for copy in raw:
        copy.start()

    def lanes(chip):
        return aligned(chip * CHIP_PATHS, CHIP_PATHS)

    def curve_copy(i):
        ty, tx, tz = shifted(i, y, x, z)
        return remote(
            store.at[0, :, :, lanes(chip_index(ty, tx, tz))],
            got.at[me],
            a_send.at[i],
            a_recv.at[me],
            device(ty, tx, tz, core),
        )

    def launch(i, carry):
        curve_copy(i).start()
        return carry

    lax.fori_loop(1, 64, launch, 0)
    own_copy = pltpu.make_async_copy(store.at[0, :, :, lanes(me)], got.at[me], own_sem)
    own_copy.start()

    def table_copy(n, slot, q):
        rows = aligned(q * CHUNK, CHUNK)
        return remote(tables.at[slot, rows, :], tables.at[slot, rows, :], p_send.at[n], p_recv.at[n], partner)

    for copy in own_raw:
        copy.wait()

    def build(j, carry):
        @pl.when(j == 1)
        def _():
            for copy in raw:
                copy.wait()

        slot = lax.rem(low + j, 2) * 2 + core
        build_table(
            raw_i, raw_a, j, slot, tables, bidx, bhi, blo, onehot, flows,
            lambda q: table_copy(j * CHUNKS + q, slot, q).start(),
        )
        return carry

    lax.fori_loop(0, 2, build, 0)

    def landed(i, carry):
        curve_copy(i).wait_send()
        ty, tx, tz = shifted(i, y, x, z)
        source = chip_index(ty, tx, tz)
        remote(
            store.at[0, :, :, lanes(me)], got.at[source], a_send.at[i], a_recv.at[source],
            device(ty, tx, tz, core),
        ).wait_recv()
        return carry

    own_copy.wait()
    lax.fori_loop(1, 64, landed, 0)

    def pick(date, low_z):
        slot = slot_ref[date]
        place = lax.div(slot, 2)
        return got[lax.div(place, 2) * 4 + lax.rem(place, 2) * 2 + low_z, lax.rem(slot, 2)]

    for k in range(HALF):
        for low_z in range(2):
            give[low_z, k] = pick((1 - core) * HALF + k, low_z)
    trade = remote(give, curves.at[core], c_send, c_recv, partner)
    trade.start()
    for k in range(HALF):
        for low_z in range(2):
            curves[core, low_z, k] = pick(core * HALF + k, low_z)
    trade.wait_send()
    remote(give, curves.at[1 - core], c_send, c_recv, partner).wait_recv()
    for j in range(2):
        slot = lax.rem(low + j, 2) * 2 + core
        theirs = lax.rem(low + j, 2) * 2 + 1 - core
        for q in range(CHUNKS):
            table_copy(j * CHUNKS + q, slot, q).wait_send()
            table_copy(j * CHUNKS + q, theirs, q).wait_recv()

    price(core, tables, curves, weight_ref, part, discount, value, slope, pull, mesh_w)

    def stage(source_of, buf, send, recv, here, others, device_of):
        sends = []
        for i, t in enumerate(others):
            copy = remote(source_of(t), buf.at[here], send.at[i], recv.at[here], device_of(t))
            copy.start()
            sends.append(copy)
        for i, t in enumerate(others):
            sends[i].wait_send()
            remote(source_of(here), buf.at[t], send.at[i], recv.at[t], device_of(t)).wait_recv()

    z_buf[z] = part[low]
    stage(
        lambda t: part.at[lax.rem(t, 2)], z_buf, z_send, z_recv, z, in_z,
        lambda t: device(y, x, t, core),
    )
    y_buf[y] = (z_buf[0] + z_buf[1]) + (z_buf[2] + z_buf[3])
    stage(lambda t: y_buf.at[y], y_buf, y_send, y_recv, y, in_y, lambda t: device(t, x, z, core))
    both = (y_buf[0] + y_buf[1]) + (y_buf[2] + y_buf[3])
    give_x = z_buf.at[0]
    give_x[...] = both
    sends = []
    for i, t in enumerate([x] + in_x):
        for c in range(2):
            if i == 0 and c == 0:
                continue
            to_core = lax.rem(core + c, 2)
            copy = remote(
                give_x.at[to_core], x_buf.at[core, x], x_send.at[2 * i + c], x_recv.at[core, x],
                device(y, t, z, to_core),
            )
            copy.start()
            sends.append((copy, t, to_core, 2 * i + c))
    x_buf[core, x] = give_x[core]
    for copy, t, from_core, n in sends:
        copy.wait_send()
        remote(
            give_x.at[core], x_buf.at[from_core, t], x_send.at[n], x_recv.at[from_core, t],
            device(y, t, z, from_core),
        ).wait_recv()
    for half in range(2):
        out[half] = (x_buf[half, 0] + x_buf[half, 1]) + (x_buf[half, 2] + x_buf[half, 3])


def local(curve_store, cash_index, cash_amount, trade_set, date_slot, default_weight):
    taps = jnp.concatenate(
        [cash_index[0].T, trade_set, jnp.zeros((TAPS - NCF - 1, TRADES), jnp.int32)], axis=0
    )
    whole = pl.BlockSpec(memory_space=pltpu.VMEM)
    there = pl.BlockSpec(memory_space=pl.ANY)
    dma = pltpu.SemaphoreType.DMA
    quarter = (2 * HALF, 128)
    sums = pl.pallas_call(
        kernel,
        out_shape=jax.ShapeDtypeStruct((2, *quarter), F32),
        in_specs=[pl.BlockSpec(memory_space=pltpu.SMEM), there, there, there, whole],
        out_specs=whole,
        scratch_shapes=[
            pltpu.VMEM((64, 2, NODES, CHIP_PATHS), BF),
            pltpu.VMEM((2, 2, HALF, NODES, CHIP_PATHS), BF),
            pltpu.VMEM((2, HALF, NODES, CHIP_PATHS), BF),
            pltpu.VMEM((2, TAPS, TRADES), jnp.int32),
            pltpu.VMEM((2, NCF, TRADES), F32),
            pltpu.VMEM((NCF, 16, TRADES), BF),
            pltpu.VMEM((NCF, 16, TRADES), BF),
            pltpu.VMEM((NCF, 16, TRADES), BF),
            pltpu.VMEM((NSETS, TRADES), BF),
            pltpu.VMEM((2 * CHUNK, TRADES), BF),
            pltpu.VMEM((4, CFG, NSETS), BF),
            pltpu.VMEM((ROWS, 4 * CFG), BF),
            pltpu.VMEM((ROWS, NSETS), F32),
            pltpu.VMEM((ROWS, NSETS), BF),
            pltpu.VMEM((HALF, 8, CFG), F32),
            pltpu.VMEM((HALF, NODES, CFG), BF),
            pltpu.VMEM((2, 2, *quarter), F32),
            pltpu.VMEM((4, 2, *quarter), F32),
            pltpu.VMEM((4, 2, *quarter), F32),
            pltpu.VMEM((2, 4, *quarter), F32),
            dma((64,)),
            dma((64,)),
            dma,
            dma((2,)),
            dma((4,)),
            dma((4,)),
            dma((2 * CHUNKS,)),
            dma((2 * CHUNKS,)),
            dma,
            dma,
            dma((3,)),
            dma((4,)),
            dma((3,)),
            dma((4,)),
            dma((8,)),
            dma((2, 4)),
        ],
        compiler_params=pltpu.CompilerParams(
            collective_id=0, has_side_effects=True, vmem_limit_bytes=60 * 1024 * 1024
        ),
    )(date_slot, curve_store, taps, cash_amount[0].T, default_weight)
    exposure = sums[:, :HALF].reshape(DATES, NSETS // 4)
    sens = sums[:, HALF:, :NODES].reshape(1, DATES, NODES)
    return exposure, sens


def solution(mesh):
    in_specs = (
        P("ccy", "path", None, None),
        P("ccy", None, None),
        P("ccy", None, None),
        P("ccy", None),
        P(),
        P(),
    )
    out_specs = (P(None, "ccy"), P("ccy", None, None))
    return jax.shard_map(local, mesh=mesh, in_specs=in_specs, out_specs=out_specs, check_vma=False)
```

```python
import jax
import jax.numpy as jnp
from jax import lax
from jax.experimental import pallas as pl
from jax.experimental.pallas import tpu as pltpu
from jax.sharding import PartitionSpec as P

NODES = 64
CFG = 1024
NSETS = 512
NCF = 16
TRADES = 2048
DATES = 16
HALF = DATES // 2
CHIP_PATHS = 128
ROWS = HALF * CHIP_PATHS
TOTAL_PATHS = 8192
SOFTEN = 0.04
LOG2E = 1.4426950408889634
CHUNK = 256
CHUNKS = CFG // CHUNK
TAPS = 24
MESH = pl.DeviceIdType.MESH
BF = jnp.bfloat16
F32 = jnp.float32
NT = (((1,), (1,)), ((), ()))
TN = (((0,), (0,)), ((), ()))


def coords():
    ccy = lax.axis_index("ccy")
    path = lax.axis_index("path")
    core = lax.rem(ccy, 2)
    z = lax.rem(path, 2) * 2 + lax.div(ccy, 2)
    x = lax.rem(lax.div(path, 2), 4)
    y = lax.div(path, 8)
    return y, x, z, core


def device(y, x, z, core):
    return (lax.rem(z, 2) * 2 + core, (y * 4 + x) * 2 + lax.div(z, 2))


def chip_index(y, x, z):
    return (y * 4 + x) * 4 + z


def shifted(i, y, x, z):
    b, c, a = lax.div(i, 16), lax.rem(lax.div(i, 4), 4), lax.rem(i, 4)
    return (
        lax.rem(y + a, 4),
        lax.rem(x + a + b, 4),
        lax.rem(z + a + c, 4),
    )


def remote(src, dst, send, recv, target):
    return pltpu.make_async_remote_copy(
        src_ref=src,
        dst_ref=dst,
        send_sem=send,
        recv_sem=recv,
        device_id=target,
        device_id_type=MESH,
    )


def aligned(start, size):
    return pl.ds(pl.multiple_of(start, size), size)


def grid_tables(date, nodes):
    steps = lax.broadcasted_iota(jnp.int32, (1, CFG), 1) + 1 - 16 * (date + 1)
    steps = steps.astype(F32)
    place = jnp.clip(steps * (1.0 / 16.0), 1.0, float(NODES))
    node = (lax.broadcasted_iota(jnp.int32, (nodes, CFG), 0) + 1).astype(F32)
    weights = jnp.maximum(0.0, 1.0 - jnp.abs(place - node))
    return steps, steps * (1.0 / 32.0), weights


def prepare_trades(raw_i, raw_a, j, merged, onehot):
    amounts = raw_a[j]
    indices = raw_i[j, pl.ds(0, NCF), :]
    sums = jnp.zeros_like(amounts)
    for k in range(NCF):
        sums = sums + jnp.where(indices == indices[k : k + 1], amounts[k : k + 1], 0.0)
    merged[j] = sums
    sets = raw_i[j, pl.ds(NCF, 1), :]
    for s in range(0, NSETS, 64):
        ids = lax.broadcasted_iota(jnp.int32, (64, TRADES), 0) + s
        onehot[j, pl.ds(s, 64), :] = jnp.where(ids == sets, 1.0, 0.0).astype(BF)


def spread(raw_i, merged, j, base, start, flows):
    cols = pl.ds(start, 128)
    for part in range(0, CHUNK, 128):
        ids = [lax.broadcasted_iota(jnp.int32, (8, 128), 0) + (base + part + 8 * r) for r in range(16)]
        accs = [jnp.zeros((8, 128), F32)] * 16
        for k in range(NCF):
            where = jnp.broadcast_to(raw_i[j, pl.ds(k, 1), cols], (8, 128))
            worth = jnp.broadcast_to(merged[j, pl.ds(k, 1), cols], (8, 128))
            accs = [jnp.where(i == where, worth, acc) for i, acc in zip(ids, accs)]
        for r in range(0, 16, 2):
            total = jnp.concatenate(accs[r : r + 2], axis=0)
            high = total.astype(BF)
            flows[pl.ds(part + 8 * r, 16), cols] = high
            flows[pl.ds(CHUNK + part + 8 * r, 16), cols] = (total - high.astype(F32)).astype(BF)


def price(core, tables, curves, weight_ref, part, discount, value, slope, pull, mesh_w):
    for k in range(HALF):
        pull[k] = jnp.zeros((8, CFG), F32)
    part[...] = jnp.zeros_like(part)

    def discounts(k, carry):
        steps, remain, weights = grid_tables(core * HALF + k, NODES)
        weights = weights.astype(BF)
        mesh_w[k] = weights
        down = remain * -LOG2E
        live = steps[:, :256] > 0.0
        for g in range(4):
            rate = lax.dot_general(curves[g % 2, g // 2, k], weights, TN, preferred_element_type=F32)
            held = jnp.exp2(rate * down)
            rows = aligned(k * CHIP_PATHS, CHIP_PATHS)
            discount[rows, pl.ds(g * CFG, 256)] = jnp.where(live, held[:, :256], 0.0).astype(BF)
            discount[rows, pl.ds(g * CFG + 256, CFG - 256)] = held[:, 256:].astype(BF)
        return carry

    lax.fori_loop(0, HALF, discounts, 0)

    value[...] = jnp.dot(discount[:, pl.ds(0, CFG)], tables[0], preferred_element_type=F32)

    def add_group(g, carry):
        value[...] += jnp.dot(discount[:, aligned(g * CFG, CFG)], tables[g], preferred_element_type=F32)
        return carry

    lax.fori_loop(1, 4, add_group, 0)

    def slopes(k, carry):
        rows = aligned(k * CHIP_PATHS, CHIP_PATHS)
        v = value[rows, :]
        square = v * v + SOFTEN
        inverse = lax.rsqrt(square)
        mean = jnp.sum(0.5 * (v + square * inverse), axis=0, keepdims=True) * (1.0 / TOTAL_PATHS)
        scale = weight_ref[pl.ds(core * HALF + k, 1), :] * (0.5 / TOTAL_PATHS)
        slope[rows, :] = (scale * (1.0 + v * inverse)).astype(BF)
        for i in range(4):
            part[i // 2, i % 2, pl.ds(k, 1), :] = mean[:, i * 128 : (i + 1) * 128]
        return carry

    lax.fori_loop(0, HALF, slopes, 0)

    def pull_group(n, carry):
        g, c = lax.div(n, CHUNKS), lax.rem(n, CHUNKS)
        cash = tables[g, aligned(c * CHUNK, CHUNK), :]
        back = lax.dot_general(slope[...], cash, NT, preferred_element_type=F32)
        weighed = back * discount[:, aligned(n * CHUNK, CHUNK)].astype(F32)
        sums = weighed.reshape(HALF, CHIP_PATHS, CHUNK).sum(axis=1)
        for k in range(HALF):
            pull[k, pl.ds(g, 1), aligned(c * CHUNK, CHUNK)] = sums[k : k + 1]
        return carry

    lax.fori_loop(0, 4 * CHUNKS, pull_group, 0)

    for k in range(HALF):
        _, remain, _ = grid_tables(core * HALF + k, 8)
        rest = pull[k] * (remain * -1.0)
        pieces = []
        for _ in range(3):
            piece = rest.astype(BF).astype(F32)
            rest = rest - piece
            pieces.append(piece)
        pieces.append(jnp.zeros_like(rest))
        stack = jnp.concatenate(pieces, axis=0).astype(BF)
        sums = lax.dot_general(stack, mesh_w[k], NT, preferred_element_type=F32)
        total = sums[:8] + sums[8:16] + sums[16:24]
        for g in range(4):
            part[g // 2, g % 2, pl.ds(HALF + k, 1), pl.ds(0, NODES)] = total[g : g + 1]


def kernel(
    slot_ref, store, taps, amounts, weight_ref,
    out,
    got, curves, give, raw_i, raw_a, merged, onehot, flows, tables,
    discount, value, slope, pull, mesh_w, part, z_buf, y_buf, x_buf,
    a_send, a_recv, own_sem, l_sem, r_send, r_recv, p_send, p_recv, c_send, c_recv,
    z_send, z_recv, y_send, y_recv, x_send, x_recv,
):
    y, x, z, core = coords()
    low = lax.rem(z, 2)
    group = low * 2 + core
    other = (1 - low) * 2 + core
    partner = device(y, x, z, 1 - core)
    up = device(y, x, lax.rem(z + 1, 4), core)
    down = device(y, x, lax.rem(z + 3, 4), core)
    me = chip_index(y, x, z)
    in_z = [lax.rem(z + i, 4) for i in range(1, 4)]
    in_y = [lax.rem(y + i, 4) for i in range(1, 4)]
    in_x = [lax.rem(x + i, 4) for i in range(1, 4)]

    barrier = pltpu.get_barrier_semaphore()

    def greet(i, carry):
        pl.semaphore_signal(
            barrier, inc=1, device_id=device(*shifted(i, y, x, z), core), device_id_type=MESH
        )
        return carry

    pl.semaphore_signal(barrier, inc=1, device_id=partner, device_id_type=MESH)
    for t in in_x:
        pl.semaphore_signal(barrier, inc=1, device_id=device(y, t, z, 1 - core), device_id_type=MESH)
    lax.fori_loop(1, 64, greet, 0)
    own_raw = [
        pltpu.make_async_copy(taps, raw_i.at[0], l_sem.at[0]),
        pltpu.make_async_copy(amounts, raw_a.at[0], l_sem.at[1]),
    ]
    for copy in own_raw:
        copy.start()
    for copy in own_raw:
        copy.wait()
    prepare_trades(raw_i, raw_a, 0, merged, onehot)

    halves = [pl.ds(0, TRADES // 2), pl.ds(TRADES // 2, TRADES // 2)]
    raw = []
    for h, target in enumerate((up, down)):
        raw.append(remote(taps.at[:, halves[h]], raw_i.at[1, :, halves[h]], r_send.at[2 * h], r_recv.at[2 * h], target))
        raw.append(
            remote(amounts.at[:, halves[h]], raw_a.at[1, :, halves[h]], r_send.at[2 * h + 1], r_recv.at[2 * h + 1], target)
        )

    def lanes(chip):
        return aligned(chip * CHIP_PATHS, CHIP_PATHS)

    def curve_copy(i):
        ty, tx, tz = shifted(i, y, x, z)
        return remote(
            store.at[0, :, :, lanes(chip_index(ty, tx, tz))],
            got.at[me],
            a_send.at[i],
            a_recv.at[me],
            device(ty, tx, tz, core),
        )

    def launch(i, carry):
        curve_copy(i).start()
        return carry

    own_copy = pltpu.make_async_copy(store.at[0, :, :, lanes(me)], got.at[me], own_sem)
    own_copy.start()

    def table_copy(n, slot, q):
        rows = aligned(q * CHUNK, CHUNK)
        return remote(tables.at[slot, rows, :], tables.at[slot, rows, :], p_send.at[n], p_recv.at[n], partner)

    def build(n, carry):
        @pl.when(n == 1)
        def _():
            pl.semaphore_wait(barrier, 67)
            for copy in raw:
                copy.start()
            lax.fori_loop(1, 64, launch, 0)
            table_copy(0, group, 0).start()

        @pl.when(n == CHUNKS)
        def _():
            for copy in raw:
                copy.wait()
            prepare_trades(raw_i, raw_a, 1, merged, onehot)

        j, q = lax.div(n, CHUNKS), lax.rem(n, CHUNKS)
        slot = lax.rem(low + j, 2) * 2 + core
        for t in range(0, TRADES, 128):
            spread(raw_i, merged, j, q * CHUNK, t, flows)
        both = lax.dot_general(flows[...], onehot[j], NT, preferred_element_type=F32)
        tables[slot, aligned(q * CHUNK, CHUNK), :] = (both[:CHUNK] + both[CHUNK:]).astype(BF)

        @pl.when(n > 0)
        def _():
            table_copy(n, slot, q).start()

        return carry

    lax.fori_loop(0, 2 * CHUNKS, build, 0)

    def landed(i, carry):
        curve_copy(i).wait_send()
        ty, tx, tz = shifted(i, y, x, z)
        source = chip_index(ty, tx, tz)
        remote(
            store.at[0, :, :, lanes(me)], got.at[source], a_send.at[i], a_recv.at[source],
            device(ty, tx, tz, core),
        ).wait_recv()
        return carry

    own_copy.wait()
    lax.fori_loop(1, 64, landed, 0)

    def pick(date, low_z):
        slot = slot_ref[date]
        place = lax.div(slot, 2)
        return got[lax.div(place, 2) * 4 + lax.rem(place, 2) * 2 + low_z, lax.rem(slot, 2)]

    for k in range(HALF):
        for low_z in range(2):
            give[low_z, k] = pick((1 - core) * HALF + k, low_z)
    trade = remote(give, curves.at[core], c_send, c_recv, partner)
    trade.start()
    for k in range(HALF):
        for low_z in range(2):
            curves[core, low_z, k] = pick(core * HALF + k, low_z)
    trade.wait_send()
    remote(give, curves.at[1 - core], c_send, c_recv, partner).wait_recv()
    for j in range(2):
        slot = lax.rem(low + j, 2) * 2 + core
        theirs = lax.rem(low + j, 2) * 2 + 1 - core
        for q in range(CHUNKS):
            table_copy(j * CHUNKS + q, slot, q).wait_send()
            table_copy(j * CHUNKS + q, theirs, q).wait_recv()

    price(core, tables, curves, weight_ref, part, discount, value, slope, pull, mesh_w)

    def stage(source_of, buf, send, recv, here, others, device_of):
        sends = []
        for i, t in enumerate(others):
            copy = remote(source_of(t), buf.at[here], send.at[i], recv.at[here], device_of(t))
            copy.start()
            sends.append(copy)
        for i, t in enumerate(others):
            sends[i].wait_send()
            remote(source_of(here), buf.at[t], send.at[i], recv.at[t], device_of(t)).wait_recv()

    z_buf[z] = part[low]
    stage(
        lambda t: part.at[lax.rem(t, 2)], z_buf, z_send, z_recv, z, in_z,
        lambda t: device(y, x, t, core),
    )
    y_buf[y] = (z_buf[0] + z_buf[1]) + (z_buf[2] + z_buf[3])
    stage(lambda t: y_buf.at[y], y_buf, y_send, y_recv, y, in_y, lambda t: device(t, x, z, core))
    both = (y_buf[0] + y_buf[1]) + (y_buf[2] + y_buf[3])
    give_x = z_buf.at[0]
    give_x[...] = both
    sends = []
    for i, t in enumerate([x] + in_x):
        for c in range(2):
            if i == 0 and c == 0:
                continue
            to_core = lax.rem(core + c, 2)
            copy = remote(
                give_x.at[to_core], x_buf.at[core, x], x_send.at[2 * i + c], x_recv.at[core, x],
                device(y, t, z, to_core),
            )
            copy.start()
            sends.append((copy, t, to_core, 2 * i + c))
    x_buf[core, x] = give_x[core]
    for copy, t, from_core, n in sends:
        copy.wait_send()
        remote(
            give_x.at[core], x_buf.at[from_core, t], x_send.at[n], x_recv.at[from_core, t],
            device(y, t, z, from_core),
        ).wait_recv()
    for half in range(2):
        out[half] = (x_buf[half, 0] + x_buf[half, 1]) + (x_buf[half, 2] + x_buf[half, 3])


def local(curve_store, cash_index, cash_amount, trade_set, date_slot, default_weight):
    taps = jnp.concatenate(
        [cash_index[0].T, trade_set, jnp.zeros((TAPS - NCF - 1, TRADES), jnp.int32)], axis=0
    )
    whole = pl.BlockSpec(memory_space=pltpu.VMEM)
    there = pl.BlockSpec(memory_space=pl.ANY)
    dma = pltpu.SemaphoreType.DMA
    quarter = (2 * HALF, 128)
    sums = pl.pallas_call(
        kernel,
        out_shape=jax.ShapeDtypeStruct((2, *quarter), F32),
        in_specs=[pl.BlockSpec(memory_space=pltpu.SMEM), there, there, there, whole],
        out_specs=whole,
        scratch_shapes=[
            pltpu.VMEM((64, 2, NODES, CHIP_PATHS), BF),
            pltpu.VMEM((2, 2, HALF, NODES, CHIP_PATHS), BF),
            pltpu.VMEM((2, HALF, NODES, CHIP_PATHS), BF),
            pltpu.VMEM((2, TAPS, TRADES), jnp.int32),
            pltpu.VMEM((2, NCF, TRADES), F32),
            pltpu.VMEM((2, NCF, TRADES), F32),
            pltpu.VMEM((2, NSETS, TRADES), BF),
            pltpu.VMEM((2 * CHUNK, TRADES), BF),
            pltpu.VMEM((4, CFG, NSETS), BF),
            pltpu.VMEM((ROWS, 4 * CFG), BF),
            pltpu.VMEM((ROWS, NSETS), F32),
            pltpu.VMEM((ROWS, NSETS), BF),
            pltpu.VMEM((HALF, 8, CFG), F32),
            pltpu.VMEM((HALF, NODES, CFG), BF),
            pltpu.VMEM((2, 2, *quarter), F32),
            pltpu.VMEM((4, 2, *quarter), F32),
            pltpu.VMEM((4, 2, *quarter), F32),
            pltpu.VMEM((2, 4, *quarter), F32),
            dma((64,)),
            dma((64,)),
            dma,
            dma((2,)),
            dma((4,)),
            dma((4,)),
            dma((2 * CHUNKS,)),
            dma((2 * CHUNKS,)),
            dma,
            dma,
            dma((3,)),
            dma((4,)),
            dma((3,)),
            dma((4,)),
            dma((8,)),
            dma((2, 4)),
        ],
        compiler_params=pltpu.CompilerParams(
            collective_id=0, has_side_effects=True, vmem_limit_bytes=60 * 1024 * 1024
        ),
    )(date_slot, curve_store, taps, cash_amount[0].T, default_weight)
    exposure = sums[:, :HALF].reshape(DATES, NSETS // 4)
    sens = sums[:, HALF:, :NODES].reshape(1, DATES, NODES)
    return exposure, sens


def solution(mesh):
    in_specs = (
        P("ccy", "path", None, None),
        P("ccy", None, None),
        P("ccy", None, None),
        P("ccy", None),
        P(),
        P(),
    )
    out_specs = (P(None, "ccy"), P("ccy", None, None))
    return jax.shard_map(local, mesh=mesh, in_specs=in_specs, out_specs=out_specs, check_vma=False)
```

```python
import jax
import jax.numpy as jnp
from jax import lax
from jax.experimental import pallas as pl
from jax.experimental.pallas import tpu as pltpu
from jax.sharding import PartitionSpec as P

NODES = 64
CFG = 1024
NSETS = 512
NCF = 16
TRADES = 2048
DATES = 16
HALF = DATES // 2
CHIP_PATHS = 128
ROWS = HALF * CHIP_PATHS
TOTAL_PATHS = 8192
SOFTEN = 0.04
LOG2E = 1.4426950408889634
CHUNK = 256
CHUNKS = CFG // CHUNK
TAPS = 24
MESH = pl.DeviceIdType.MESH
BF = jnp.bfloat16
F32 = jnp.float32
NT = (((1,), (1,)), ((), ()))
TN = (((0,), (0,)), ((), ()))


def coords():
    ccy = lax.axis_index("ccy")
    path = lax.axis_index("path")
    core = lax.rem(ccy, 2)
    z = lax.rem(path, 2) * 2 + lax.div(ccy, 2)
    x = lax.rem(lax.div(path, 2), 4)
    y = lax.div(path, 8)
    return y, x, z, core


def device(y, x, z, core):
    return (lax.rem(z, 2) * 2 + core, (y * 4 + x) * 2 + lax.div(z, 2))


def chip_index(y, x, z):
    return (y * 4 + x) * 4 + z


def shifted(i, y, x, z):
    b, c, a = lax.div(i, 16), lax.rem(lax.div(i, 4), 4), lax.rem(i, 4)
    return (
        lax.rem(y + a, 4),
        lax.rem(x + a + b, 4),
        lax.rem(z + a + c, 4),
    )


def remote(src, dst, send, recv, target):
    return pltpu.make_async_remote_copy(
        src_ref=src,
        dst_ref=dst,
        send_sem=send,
        recv_sem=recv,
        device_id=target,
        device_id_type=MESH,
    )


def aligned(start, size):
    return pl.ds(pl.multiple_of(start, size), size)


def grid_tables(date, nodes):
    steps = lax.broadcasted_iota(jnp.int32, (1, CFG), 1) + 1 - 16 * (date + 1)
    steps = steps.astype(F32)
    place = jnp.clip(steps * (1.0 / 16.0), 1.0, float(NODES))
    node = (lax.broadcasted_iota(jnp.int32, (nodes, CFG), 0) + 1).astype(F32)
    weights = jnp.maximum(0.0, 1.0 - jnp.abs(place - node))
    return steps, steps * (1.0 / 32.0), weights


def prepare_trades(raw_i, raw_a, j, merged, onehot):
    amounts = raw_a[j]
    indices = raw_i[j, pl.ds(0, NCF), :]
    sums = jnp.zeros_like(amounts)
    for k in range(NCF):
        sums = sums + jnp.where(indices == indices[k : k + 1], amounts[k : k + 1], 0.0)
    merged[j] = sums
    sets = raw_i[j, pl.ds(NCF, 1), :]
    for s in range(0, NSETS, 64):
        ids = lax.broadcasted_iota(jnp.int32, (64, TRADES), 0) + s
        onehot[j, pl.ds(s, 64), :] = jnp.where(ids == sets, 1.0, 0.0).astype(BF)


def spread(raw_i, merged, j, base, start, flows):
    cols = pl.ds(start, 128)
    for part in range(0, CHUNK, 128):
        ids = [lax.broadcasted_iota(jnp.int32, (8, 128), 0) + (base + part + 8 * r) for r in range(16)]
        accs = [jnp.zeros((8, 128), F32)] * 16
        for k in range(NCF):
            where = jnp.broadcast_to(raw_i[j, pl.ds(k, 1), cols], (8, 128))
            worth = jnp.broadcast_to(merged[j, pl.ds(k, 1), cols], (8, 128))
            accs = [jnp.where(i == where, worth, acc) for i, acc in zip(ids, accs)]
        for r in range(0, 16, 2):
            total = jnp.concatenate(accs[r : r + 2], axis=0)
            high = total.astype(BF)
            flows[pl.ds(part + 8 * r, 16), cols] = high
            flows[pl.ds(CHUNK + part + 8 * r, 16), cols] = (total - high.astype(F32)).astype(BF)


def price(core, tables, curves, weight_ref, part, discount, value, slope, pull, mesh_w):
    for k in range(HALF):
        pull[k] = jnp.zeros((8, CFG), F32)
    part[...] = jnp.zeros_like(part)

    def discounts(k, carry):
        steps, remain, weights = grid_tables(core * HALF + k, NODES)
        weights = weights.astype(BF)
        mesh_w[k] = weights
        down = remain * -LOG2E
        live = steps[:, :256] > 0.0
        for g in range(4):
            rate = lax.dot_general(curves[g % 2, g // 2, k], weights, TN, preferred_element_type=F32)
            held = jnp.exp2(rate * down)
            rows = aligned(k * CHIP_PATHS, CHIP_PATHS)
            discount[rows, pl.ds(g * CFG, 256)] = jnp.where(live, held[:, :256], 0.0).astype(BF)
            discount[rows, pl.ds(g * CFG + 256, CFG - 256)] = held[:, 256:].astype(BF)
        return carry

    lax.fori_loop(0, HALF, discounts, 0)

    value[...] = jnp.dot(discount[:, pl.ds(0, CFG)], tables[0], preferred_element_type=F32)

    def add_group(g, carry):
        value[...] += jnp.dot(discount[:, aligned(g * CFG, CFG)], tables[g], preferred_element_type=F32)
        return carry

    lax.fori_loop(1, 4, add_group, 0)

    def slopes(k, carry):
        rows = aligned(k * CHIP_PATHS, CHIP_PATHS)
        v = value[rows, :]
        square = v * v + SOFTEN
        inverse = lax.rsqrt(square)
        mean = jnp.sum(0.5 * (v + square * inverse), axis=0, keepdims=True) * (1.0 / TOTAL_PATHS)
        scale = weight_ref[pl.ds(core * HALF + k, 1), :] * (0.5 / TOTAL_PATHS)
        slope[rows, :] = (scale * (1.0 + v * inverse)).astype(BF)
        for i in range(4):
            part[i // 2, i % 2, pl.ds(k, 1), :] = mean[:, i * 128 : (i + 1) * 128]
        return carry

    lax.fori_loop(0, HALF, slopes, 0)

    def pull_group(n, carry):
        g, c = lax.div(n, 2), lax.rem(n, 2)
        cash = tables[g, aligned(c * 512, 512), :]
        back = lax.dot_general(slope[...], cash, NT, preferred_element_type=F32)
        weighed = back * discount[:, aligned(n * 512, 512)].astype(F32)
        sums = weighed.reshape(HALF, CHIP_PATHS, 512).sum(axis=1)
        for k in range(HALF):
            pull[k, pl.ds(g, 1), aligned(c * 512, 512)] = sums[k : k + 1]
        return carry

    lax.fori_loop(0, 8, pull_group, 0)

    for k in range(HALF):
        _, remain, _ = grid_tables(core * HALF + k, 8)
        rest = pull[k] * (remain * -1.0)
        pieces = []
        for _ in range(3):
            piece = rest.astype(BF).astype(F32)
            rest = rest - piece
            pieces.append(piece)
        pieces.append(jnp.zeros_like(rest))
        stack = jnp.concatenate(pieces, axis=0).astype(BF)
        sums = lax.dot_general(stack, mesh_w[k], NT, preferred_element_type=F32)
        total = sums[:8] + sums[8:16] + sums[16:24]
        for g in range(4):
            part[g // 2, g % 2, pl.ds(HALF + k, 1), pl.ds(0, NODES)] = total[g : g + 1]


def kernel(
    slot_ref, store, taps, amounts, weight_ref,
    out,
    got, curves, give, raw_i, raw_a, merged, onehot, flows, tables,
    discount, value, slope, pull, mesh_w, part, z_buf, y_buf, x_buf,
    a_send, a_recv, own_sem, l_sem, r_send, r_recv, p_send, p_recv, c_send, c_recv,
    z_send, z_recv, y_send, y_recv, x_send, x_recv,
):
    y, x, z, core = coords()
    low = lax.rem(z, 2)
    group = low * 2 + core
    other = (1 - low) * 2 + core
    partner = device(y, x, z, 1 - core)
    up = device(y, x, lax.rem(z + 1, 4), core)
    down = device(y, x, lax.rem(z + 3, 4), core)
    me = chip_index(y, x, z)
    in_z = [lax.rem(z + i, 4) for i in range(1, 4)]
    in_y = [lax.rem(y + i, 4) for i in range(1, 4)]
    in_x = [lax.rem(x + i, 4) for i in range(1, 4)]

    barrier = pltpu.get_barrier_semaphore()

    def greet(i, carry):
        pl.semaphore_signal(
            barrier, inc=1, device_id=device(*shifted(i, y, x, z), core), device_id_type=MESH
        )
        return carry

    pl.semaphore_signal(barrier, inc=1, device_id=partner, device_id_type=MESH)
    for t in in_x:
        pl.semaphore_signal(barrier, inc=1, device_id=device(y, t, z, 1 - core), device_id_type=MESH)
    lax.fori_loop(1, 64, greet, 0)
    own_raw = [
        pltpu.make_async_copy(taps, raw_i.at[0], l_sem.at[0]),
        pltpu.make_async_copy(amounts, raw_a.at[0], l_sem.at[1]),
    ]
    for copy in own_raw:
        copy.start()
    for copy in own_raw:
        copy.wait()
    prepare_trades(raw_i, raw_a, 0, merged, onehot)

    halves = [pl.ds(0, TRADES // 2), pl.ds(TRADES // 2, TRADES // 2)]
    raw = []
    for h, target in enumerate((up, down)):
        raw.append(remote(taps.at[:, halves[h]], raw_i.at[1, :, halves[h]], r_send.at[2 * h], r_recv.at[2 * h], target))
        raw.append(
            remote(amounts.at[:, halves[h]], raw_a.at[1, :, halves[h]], r_send.at[2 * h + 1], r_recv.at[2 * h + 1], target)
        )

    def lanes(chip):
        return aligned(chip * CHIP_PATHS, CHIP_PATHS)

    def curve_copy(i):
        ty, tx, tz = shifted(i, y, x, z)
        return remote(
            store.at[0, :, :, lanes(chip_index(ty, tx, tz))],
            got.at[me],
            a_send.at[i],
            a_recv.at[me],
            device(ty, tx, tz, core),
        )

    def launch(i, carry):
        curve_copy(i).start()
        return carry

    own_copy = pltpu.make_async_copy(store.at[0, :, :, lanes(me)], got.at[me], own_sem)
    own_copy.start()

    def table_copy(n, slot, q):
        rows = aligned(q * CHUNK, CHUNK)
        return remote(tables.at[slot, rows, :], tables.at[slot, rows, :], p_send.at[n], p_recv.at[n], partner)

    def build(n, carry):
        @pl.when(n == 1)
        def _():
            pl.semaphore_wait(barrier, 67)
            for copy in raw:
                copy.start()
            table_copy(0, group, 0).start()

        @pl.when(n == 2)
        def _():
            lax.fori_loop(1, 64, launch, 0)

        @pl.when(n == CHUNKS)
        def _():
            for copy in raw:
                copy.wait()
            prepare_trades(raw_i, raw_a, 1, merged, onehot)

        j, q = lax.div(n, CHUNKS), lax.rem(n, CHUNKS)
        slot = lax.rem(low + j, 2) * 2 + core
        for t in range(0, TRADES, 128):
            spread(raw_i, merged, j, q * CHUNK, t, flows)
        both = lax.dot_general(flows[...], onehot[j], NT, preferred_element_type=F32)
        tables[slot, aligned(q * CHUNK, CHUNK), :] = (both[:CHUNK] + both[CHUNK:]).astype(BF)

        @pl.when(n > 0)
        def _():
            table_copy(n, slot, q).start()

        return carry

    lax.fori_loop(0, 2 * CHUNKS, build, 0)

    def landed(i, carry):
        curve_copy(i).wait_send()
        ty, tx, tz = shifted(i, y, x, z)
        source = chip_index(ty, tx, tz)
        remote(
            store.at[0, :, :, lanes(me)], got.at[source], a_send.at[i], a_recv.at[source],
            device(ty, tx, tz, core),
        ).wait_recv()
        return carry

    own_copy.wait()
    lax.fori_loop(1, 64, landed, 0)

    def pick(date, low_z):
        slot = slot_ref[date]
        place = lax.div(slot, 2)
        return got[lax.div(place, 2) * 4 + lax.rem(place, 2) * 2 + low_z, lax.rem(slot, 2)]

    for k in range(HALF):
        for low_z in range(2):
            give[low_z, k] = pick((1 - core) * HALF + k, low_z)
    trade = remote(give, curves.at[core], c_send, c_recv, partner)
    trade.start()
    for k in range(HALF):
        for low_z in range(2):
            curves[core, low_z, k] = pick(core * HALF + k, low_z)
    trade.wait_send()
    remote(give, curves.at[1 - core], c_send, c_recv, partner).wait_recv()
    for j in range(2):
        slot = lax.rem(low + j, 2) * 2 + core
        theirs = lax.rem(low + j, 2) * 2 + 1 - core
        for q in range(CHUNKS):
            table_copy(j * CHUNKS + q, slot, q).wait_send()
            table_copy(j * CHUNKS + q, theirs, q).wait_recv()

    price(core, tables, curves, weight_ref, part, discount, value, slope, pull, mesh_w)

    def stage(source_of, buf, send, recv, here, others, device_of):
        sends = []
        for i, t in enumerate(others):
            copy = remote(source_of(t), buf.at[here], send.at[i], recv.at[here], device_of(t))
            copy.start()
            sends.append(copy)
        for i, t in enumerate(others):
            sends[i].wait_send()
            remote(source_of(here), buf.at[t], send.at[i], recv.at[t], device_of(t)).wait_recv()

    z_buf[z] = part[low]
    stage(
        lambda t: part.at[lax.rem(t, 2)], z_buf, z_send, z_recv, z, in_z,
        lambda t: device(y, x, t, core),
    )
    y_buf[y] = (z_buf[0] + z_buf[1]) + (z_buf[2] + z_buf[3])
    stage(lambda t: y_buf.at[y], y_buf, y_send, y_recv, y, in_y, lambda t: device(t, x, z, core))
    both = (y_buf[0] + y_buf[1]) + (y_buf[2] + y_buf[3])
    give_x = z_buf.at[0]
    give_x[...] = both
    sends = []
    for i, t in enumerate([x] + in_x):
        for c in range(2):
            if i == 0 and c == 0:
                continue
            to_core = lax.rem(core + c, 2)
            copy = remote(
                give_x.at[to_core], x_buf.at[core, x], x_send.at[2 * i + c], x_recv.at[core, x],
                device(y, t, z, to_core),
            )
            copy.start()
            sends.append((copy, t, to_core, 2 * i + c))
    x_buf[core, x] = give_x[core]
    for copy, t, from_core, n in sends:
        copy.wait_send()
        remote(
            give_x.at[core], x_buf.at[from_core, t], x_send.at[n], x_recv.at[from_core, t],
            device(y, t, z, from_core),
        ).wait_recv()
    for half in range(2):
        out[half] = (x_buf[half, 0] + x_buf[half, 1]) + (x_buf[half, 2] + x_buf[half, 3])


def split_kernel(sums, exposure, sens):
    for half in range(2):
        exposure[pl.ds(half * HALF, HALF), :] = sums[half, :HALF]
        sens[0, pl.ds(half * HALF, HALF), :] = sums[half, HALF:, :NODES]


def local(curve_store, cash_index, cash_amount, trade_set, date_slot, default_weight):
    taps = jnp.concatenate(
        [cash_index[0].T, trade_set, jnp.zeros((TAPS - NCF - 1, TRADES), jnp.int32)], axis=0
    )
    whole = pl.BlockSpec(memory_space=pltpu.VMEM)
    there = pl.BlockSpec(memory_space=pl.ANY)
    dma = pltpu.SemaphoreType.DMA
    quarter = (2 * HALF, 128)
    sums = pl.pallas_call(
        kernel,
        out_shape=jax.ShapeDtypeStruct((2, *quarter), F32),
        in_specs=[pl.BlockSpec(memory_space=pltpu.SMEM), there, there, there, whole],
        out_specs=whole,
        scratch_shapes=[
            pltpu.VMEM((64, 2, NODES, CHIP_PATHS), BF),
            pltpu.VMEM((2, 2, HALF, NODES, CHIP_PATHS), BF),
            pltpu.VMEM((2, HALF, NODES, CHIP_PATHS), BF),
            pltpu.VMEM((2, TAPS, TRADES), jnp.int32),
            pltpu.VMEM((2, NCF, TRADES), F32),
            pltpu.VMEM((2, NCF, TRADES), F32),
            pltpu.VMEM((2, NSETS, TRADES), BF),
            pltpu.VMEM((2 * CHUNK, TRADES), BF),
            pltpu.VMEM((4, CFG, NSETS), BF),
            pltpu.VMEM((ROWS, 4 * CFG), BF),
            pltpu.VMEM((ROWS, NSETS), F32),
            pltpu.VMEM((ROWS, NSETS), BF),
            pltpu.VMEM((HALF, 8, CFG), F32),
            pltpu.VMEM((HALF, NODES, CFG), BF),
            pltpu.VMEM((2, 2, *quarter), F32),
            pltpu.VMEM((4, 2, *quarter), F32),
            pltpu.VMEM((4, 2, *quarter), F32),
            pltpu.VMEM((2, 4, *quarter), F32),
            dma((64,)),
            dma((64,)),
            dma,
            dma((2,)),
            dma((4,)),
            dma((4,)),
            dma((2 * CHUNKS,)),
            dma((2 * CHUNKS,)),
            dma,
            dma,
            dma((3,)),
            dma((4,)),
            dma((3,)),
            dma((4,)),
            dma((8,)),
            dma((2, 4)),
        ],
        compiler_params=pltpu.CompilerParams(
            collective_id=0, has_side_effects=True, vmem_limit_bytes=60 * 1024 * 1024
        ),
    )(date_slot, curve_store, taps, cash_amount[0].T, default_weight)
    return pl.pallas_call(
        split_kernel,
        out_shape=(
            jax.ShapeDtypeStruct((DATES, NSETS // 4), F32),
            jax.ShapeDtypeStruct((1, DATES, NODES), F32),
        ),
        in_specs=[whole],
        out_specs=(whole, whole),
    )(sums)


def solution(mesh):
    in_specs = (
        P("ccy", "path", None, None),
        P("ccy", None, None),
        P("ccy", None, None),
        P("ccy", None),
        P(),
        P(),
    )
    out_specs = (P(None, "ccy"), P("ccy", None, None))
    return jax.shard_map(local, mesh=mesh, in_specs=in_specs, out_specs=out_specs, check_vma=False)
```

```python
import jax
import jax.numpy as jnp
from jax import lax
from jax.experimental import pallas as pl
from jax.experimental.pallas import tpu as pltpu
from jax.sharding import PartitionSpec as P

NODES = 64
CFG = 1024
NSETS = 512
NCF = 16
TRADES = 2048
DATES = 16
HALF = DATES // 2
CHIP_PATHS = 128
ROWS = HALF * CHIP_PATHS
TOTAL_PATHS = 8192
SOFTEN = 0.04
LOG2E = 1.4426950408889634
CHUNK = 256
CHUNKS = CFG // CHUNK
TAPS = 24
MESH = pl.DeviceIdType.MESH
BF = jnp.bfloat16
F32 = jnp.float32
NT = (((1,), (1,)), ((), ()))
TN = (((0,), (0,)), ((), ()))


def coords():
    ccy = lax.axis_index("ccy")
    path = lax.axis_index("path")
    core = lax.rem(ccy, 2)
    z = lax.rem(path, 2) * 2 + lax.div(ccy, 2)
    x = lax.rem(lax.div(path, 2), 4)
    y = lax.div(path, 8)
    return y, x, z, core


def device(y, x, z, core):
    return (lax.rem(z, 2) * 2 + core, (y * 4 + x) * 2 + lax.div(z, 2))


def chip_index(y, x, z):
    return (y * 4 + x) * 4 + z


def shifted(i, y, x, z):
    b, c, a = lax.div(i, 16), lax.rem(lax.div(i, 4), 4), lax.rem(i, 4)
    return (
        lax.rem(y + a, 4),
        lax.rem(x + a + b, 4),
        lax.rem(z + a + c, 4),
    )


def remote(src, dst, send, recv, target):
    return pltpu.make_async_remote_copy(
        src_ref=src,
        dst_ref=dst,
        send_sem=send,
        recv_sem=recv,
        device_id=target,
        device_id_type=MESH,
    )


def aligned(start, size):
    if isinstance(start, int):
        return pl.ds(start, size)
    return pl.ds(pl.multiple_of(start, size), size)


def grid_tables(date, nodes):
    steps = lax.broadcasted_iota(jnp.int32, (1, CFG), 1) + 1 - 16 * (date + 1)
    steps = steps.astype(F32)
    place = jnp.clip(steps * (1.0 / 16.0), 1.0, float(NODES))
    node = (lax.broadcasted_iota(jnp.int32, (nodes, CFG), 0) + 1).astype(F32)
    weights = jnp.maximum(0.0, 1.0 - jnp.abs(place - node))
    return steps, steps * (1.0 / 32.0), weights


def prepare_trades(raw_i, raw_a, j, merged, onehot):
    amounts = raw_a[j]
    indices = raw_i[j, pl.ds(0, NCF), :]
    sums = jnp.zeros_like(amounts)
    for k in range(NCF):
        sums = sums + jnp.where(indices == indices[k : k + 1], amounts[k : k + 1], 0.0)
    merged[j] = sums
    sets = raw_i[j, pl.ds(NCF, 1), :]
    for s in range(0, NSETS, 64):
        ids = lax.broadcasted_iota(jnp.int32, (64, TRADES), 0) + s
        onehot[j, pl.ds(s, 64), :] = jnp.where(ids == sets, 1.0, 0.0).astype(BF)


def spread(raw_i, merged, j, base, start, flows):
    cols = pl.ds(start, 128)
    for part in range(0, CHUNK, 128):
        ids = [lax.broadcasted_iota(jnp.int32, (8, 128), 0) + (base + part + 8 * r) for r in range(16)]
        accs = [jnp.zeros((8, 128), F32)] * 16
        for k in range(NCF):
            where = jnp.broadcast_to(raw_i[j, pl.ds(k, 1), cols], (8, 128))
            worth = jnp.broadcast_to(merged[j, pl.ds(k, 1), cols], (8, 128))
            accs = [jnp.where(i == where, worth, acc) for i, acc in zip(ids, accs)]
        for r in range(0, 16, 2):
            total = jnp.concatenate(accs[r : r + 2], axis=0)
            high = total.astype(BF)
            flows[pl.ds(part + 8 * r, 16), cols] = high
            flows[pl.ds(CHUNK + part + 8 * r, 16), cols] = (total - high.astype(F32)).astype(BF)


def store_weights(core, mesh_w):
    for k in range(HALF):
        mesh_w[k] = grid_tables(core * HALF + k, NODES)[2].astype(BF)


def discounts(core, curves, c, discount, mesh_w):
    for k in range(HALF):
        steps, remain, _ = grid_tables(core * HALF + k, 8)
        down = remain * -LOG2E
        live = steps[:, :256] > 0.0
        rows = pl.ds(k * CHIP_PATHS, CHIP_PATHS)
        for low_z in range(2):
            rate = lax.dot_general(curves[c, low_z, k], mesh_w[k], TN, preferred_element_type=F32)
            held = jnp.exp2(rate * down)
            first = (low_z * 2 + c) * CFG
            discount[rows, aligned(first, 256)] = jnp.where(live, held[:, :256], 0.0).astype(BF)
            discount[rows, pl.ds(pl.multiple_of(first + 256, 256), CFG - 256)] = held[:, 256:].astype(BF)


def price(core, tables, weight_ref, part, discount, value, slope, pull, mesh_w):
    value[...] = jnp.dot(discount[:, pl.ds(0, CFG)], tables[0], preferred_element_type=F32)

    def add_group(g, carry):
        value[...] += jnp.dot(discount[:, aligned(g * CFG, CFG)], tables[g], preferred_element_type=F32)
        return carry

    lax.fori_loop(1, 4, add_group, 0)

    def slopes(k, carry):
        rows = aligned(k * CHIP_PATHS, CHIP_PATHS)
        v = value[rows, :]
        square = v * v + SOFTEN
        inverse = lax.rsqrt(square)
        mean = jnp.sum(0.5 * (v + square * inverse), axis=0, keepdims=True) * (1.0 / TOTAL_PATHS)
        scale = weight_ref[pl.ds(core * HALF + k, 1), :] * (0.5 / TOTAL_PATHS)
        slope[rows, :] = (scale * (1.0 + v * inverse)).astype(BF)
        for i in range(4):
            part[i // 2, i % 2, pl.ds(k, 1), :] = mean[:, i * 128 : (i + 1) * 128]
        return carry

    lax.fori_loop(0, HALF, slopes, 0)

    def pull_group(n, carry):
        g, c = lax.div(n, 2), lax.rem(n, 2)
        cash = tables[g, aligned(c * 512, 512), :]
        back = lax.dot_general(slope[...], cash, NT, preferred_element_type=F32)
        weighed = back * discount[:, aligned(n * 512, 512)].astype(F32)
        sums = weighed.reshape(HALF, CHIP_PATHS, 512).sum(axis=1)
        for k in range(HALF):
            pull[k, pl.ds(g, 1), aligned(c * 512, 512)] = sums[k : k + 1]
        return carry

    lax.fori_loop(0, 8, pull_group, 0)

    for k in range(HALF):
        _, remain, _ = grid_tables(core * HALF + k, 8)
        rest = pull[k] * (remain * -1.0)
        pieces = []
        for _ in range(3):
            piece = rest.astype(BF).astype(F32)
            rest = rest - piece
            pieces.append(piece)
        pieces.append(jnp.zeros_like(rest))
        stack = jnp.concatenate(pieces, axis=0).astype(BF)
        sums = lax.dot_general(stack, mesh_w[k], NT, preferred_element_type=F32)
        total = sums[:8] + sums[8:16] + sums[16:24]
        for g in range(4):
            part[g // 2, g % 2, pl.ds(HALF + k, 1), pl.ds(0, NODES)] = total[g : g + 1]


def kernel(
    slot_ref, store, taps, amounts, weight_ref,
    out,
    got, curves, give, raw_i, raw_a, merged, onehot, flows, tables,
    discount, value, slope, pull, mesh_w, part, z_buf, y_buf, x_buf,
    a_send, a_recv, own_sem, l_sem, r_send, r_recv, p_send, p_recv, c_send, c_recv,
    z_send, z_recv, y_send, y_recv, x_send, x_recv,
):
    y, x, z, core = coords()
    low = lax.rem(z, 2)
    group = low * 2 + core
    other = (1 - low) * 2 + core
    partner = device(y, x, z, 1 - core)
    up = device(y, x, lax.rem(z + 1, 4), core)
    down = device(y, x, lax.rem(z + 3, 4), core)
    me = chip_index(y, x, z)
    in_z = [lax.rem(z + i, 4) for i in range(1, 4)]
    in_y = [lax.rem(y + i, 4) for i in range(1, 4)]
    in_x = [lax.rem(x + i, 4) for i in range(1, 4)]

    barrier = pltpu.get_barrier_semaphore()

    def greet(i, carry):
        pl.semaphore_signal(
            barrier, inc=1, device_id=device(*shifted(i, y, x, z), core), device_id_type=MESH
        )
        return carry

    pl.semaphore_signal(barrier, inc=1, device_id=partner, device_id_type=MESH)
    for t in in_x:
        pl.semaphore_signal(barrier, inc=1, device_id=device(y, t, z, 1 - core), device_id_type=MESH)
    lax.fori_loop(1, 64, greet, 0)
    own_raw = [
        pltpu.make_async_copy(taps, raw_i.at[0], l_sem.at[0]),
        pltpu.make_async_copy(amounts, raw_a.at[0], l_sem.at[1]),
    ]
    for copy in own_raw:
        copy.start()
    for copy in own_raw:
        copy.wait()
    prepare_trades(raw_i, raw_a, 0, merged, onehot)

    halves = [pl.ds(0, TRADES // 2), pl.ds(TRADES // 2, TRADES // 2)]
    raw = []
    for h, target in enumerate((up, down)):
        raw.append(remote(taps.at[:, halves[h]], raw_i.at[1, :, halves[h]], r_send.at[2 * h], r_recv.at[2 * h], target))
        raw.append(
            remote(amounts.at[:, halves[h]], raw_a.at[1, :, halves[h]], r_send.at[2 * h + 1], r_recv.at[2 * h + 1], target)
        )

    def lanes(chip):
        return aligned(chip * CHIP_PATHS, CHIP_PATHS)

    def curve_copy(i):
        ty, tx, tz = shifted(i, y, x, z)
        return remote(
            store.at[0, :, :, lanes(chip_index(ty, tx, tz))],
            got.at[me],
            a_send.at[i],
            a_recv.at[me],
            device(ty, tx, tz, core),
        )

    def launch(i, carry):
        curve_copy(i).start()
        return carry

    own_copy = pltpu.make_async_copy(store.at[0, :, :, lanes(me)], got.at[me], own_sem)
    own_copy.start()

    def table_copy(n, slot, q):
        rows = aligned(q * CHUNK, CHUNK)
        return remote(tables.at[slot, rows, :], tables.at[slot, rows, :], p_send.at[n], p_recv.at[n], partner)

    def build(n, carry):
        @pl.when(n == 1)
        def _():
            pl.semaphore_wait(barrier, 67)
            for copy in raw:
                copy.start()
            table_copy(0, group, 0).start()

        @pl.when(n == 2)
        def _():
            lax.fori_loop(1, 64, launch, 0)

        @pl.when(n == CHUNKS)
        def _():
            for copy in raw:
                copy.wait()
            prepare_trades(raw_i, raw_a, 1, merged, onehot)

        j, q = lax.div(n, CHUNKS), lax.rem(n, CHUNKS)
        slot = lax.rem(low + j, 2) * 2 + core
        for t in range(0, TRADES, 128):
            spread(raw_i, merged, j, q * CHUNK, t, flows)
        both = lax.dot_general(flows[...], onehot[j], NT, preferred_element_type=F32)
        tables[slot, aligned(q * CHUNK, CHUNK), :] = (both[:CHUNK] + both[CHUNK:]).astype(BF)

        @pl.when(n > 0)
        def _():
            table_copy(n, slot, q).start()

        return carry

    lax.fori_loop(0, 2 * CHUNKS, build, 0)

    def landed(i, carry):
        curve_copy(i).wait_send()
        ty, tx, tz = shifted(i, y, x, z)
        source = chip_index(ty, tx, tz)
        remote(
            store.at[0, :, :, lanes(me)], got.at[source], a_send.at[i], a_recv.at[source],
            device(ty, tx, tz, core),
        ).wait_recv()
        return carry

    store_weights(core, mesh_w)
    for k in range(HALF):
        pull[k] = jnp.zeros((8, CFG), F32)
    part[...] = jnp.zeros_like(part)
    own_copy.wait()
    lax.fori_loop(1, 64, landed, 0)

    def pick(date, low_z):
        slot = slot_ref[date]
        place = lax.div(slot, 2)
        return got[lax.div(place, 2) * 4 + lax.rem(place, 2) * 2 + low_z, lax.rem(slot, 2)]

    for k in range(HALF):
        for low_z in range(2):
            give[low_z, k] = pick((1 - core) * HALF + k, low_z)
    trade = remote(give, curves.at[core], c_send, c_recv, partner)
    trade.start()
    for k in range(HALF):
        for low_z in range(2):
            curves[core, low_z, k] = pick(core * HALF + k, low_z)
    discounts(core, curves, core, discount, mesh_w)
    trade.wait_send()
    remote(give, curves.at[1 - core], c_send, c_recv, partner).wait_recv()
    discounts(core, curves, 1 - core, discount, mesh_w)
    for j in range(2):
        slot = lax.rem(low + j, 2) * 2 + core
        theirs = lax.rem(low + j, 2) * 2 + 1 - core
        for q in range(CHUNKS):
            table_copy(j * CHUNKS + q, slot, q).wait_send()
            table_copy(j * CHUNKS + q, theirs, q).wait_recv()

    price(core, tables, weight_ref, part, discount, value, slope, pull, mesh_w)

    def stage(source_of, buf, send, recv, here, others, device_of):
        sends = []
        for i, t in enumerate(others):
            copy = remote(source_of(t), buf.at[here], send.at[i], recv.at[here], device_of(t))
            copy.start()
            sends.append(copy)
        for i, t in enumerate(others):
            sends[i].wait_send()
            remote(source_of(here), buf.at[t], send.at[i], recv.at[t], device_of(t)).wait_recv()

    z_buf[z] = part[low]
    stage(
        lambda t: part.at[lax.rem(t, 2)], z_buf, z_send, z_recv, z, in_z,
        lambda t: device(y, x, t, core),
    )
    y_buf[y] = (z_buf[0] + z_buf[1]) + (z_buf[2] + z_buf[3])
    stage(lambda t: y_buf.at[y], y_buf, y_send, y_recv, y, in_y, lambda t: device(t, x, z, core))
    both = (y_buf[0] + y_buf[1]) + (y_buf[2] + y_buf[3])
    give_x = z_buf.at[0]
    give_x[...] = both
    sends = []
    for i, t in enumerate([x] + in_x):
        for c in range(2):
            if i == 0 and c == 0:
                continue
            to_core = lax.rem(core + c, 2)
            copy = remote(
                give_x.at[to_core], x_buf.at[core, x], x_send.at[2 * i + c], x_recv.at[core, x],
                device(y, t, z, to_core),
            )
            copy.start()
            sends.append((copy, t, to_core, 2 * i + c))
    x_buf[core, x] = give_x[core]
    for copy, t, from_core, n in sends:
        copy.wait_send()
        remote(
            give_x.at[core], x_buf.at[from_core, t], x_send.at[n], x_recv.at[from_core, t],
            device(y, t, z, from_core),
        ).wait_recv()
    for half in range(2):
        out[half] = (x_buf[half, 0] + x_buf[half, 1]) + (x_buf[half, 2] + x_buf[half, 3])


def split_kernel(sums, exposure, sens):
    for half in range(2):
        exposure[pl.ds(half * HALF, HALF), :] = sums[half, :HALF]
        sens[0, pl.ds(half * HALF, HALF), :] = sums[half, HALF:, :NODES]


def local(curve_store, cash_index, cash_amount, trade_set, date_slot, default_weight):
    taps = jnp.concatenate(
        [cash_index[0].T, trade_set, jnp.zeros((TAPS - NCF - 1, TRADES), jnp.int32)], axis=0
    )
    whole = pl.BlockSpec(memory_space=pltpu.VMEM)
    there = pl.BlockSpec(memory_space=pl.ANY)
    dma = pltpu.SemaphoreType.DMA
    quarter = (2 * HALF, 128)
    sums = pl.pallas_call(
        kernel,
        out_shape=jax.ShapeDtypeStruct((2, *quarter), F32),
        in_specs=[pl.BlockSpec(memory_space=pltpu.SMEM), there, there, there, whole],
        out_specs=whole,
        scratch_shapes=[
            pltpu.VMEM((64, 2, NODES, CHIP_PATHS), BF),
            pltpu.VMEM((2, 2, HALF, NODES, CHIP_PATHS), BF),
            pltpu.VMEM((2, HALF, NODES, CHIP_PATHS), BF),
            pltpu.VMEM((2, TAPS, TRADES), jnp.int32),
            pltpu.VMEM((2, NCF, TRADES), F32),
            pltpu.VMEM((2, NCF, TRADES), F32),
            pltpu.VMEM((2, NSETS, TRADES), BF),
            pltpu.VMEM((2 * CHUNK, TRADES), BF),
            pltpu.VMEM((4, CFG, NSETS), BF),
            pltpu.VMEM((ROWS, 4 * CFG), BF),
            pltpu.VMEM((ROWS, NSETS), F32),
            pltpu.VMEM((ROWS, NSETS), BF),
            pltpu.VMEM((HALF, 8, CFG), F32),
            pltpu.VMEM((HALF, NODES, CFG), BF),
            pltpu.VMEM((2, 2, *quarter), F32),
            pltpu.VMEM((4, 2, *quarter), F32),
            pltpu.VMEM((4, 2, *quarter), F32),
            pltpu.VMEM((2, 4, *quarter), F32),
            dma((64,)),
            dma((64,)),
            dma,
            dma((2,)),
            dma((4,)),
            dma((4,)),
            dma((2 * CHUNKS,)),
            dma((2 * CHUNKS,)),
            dma,
            dma,
            dma((3,)),
            dma((4,)),
            dma((3,)),
            dma((4,)),
            dma((8,)),
            dma((2, 4)),
        ],
        compiler_params=pltpu.CompilerParams(
            collective_id=0, has_side_effects=True, vmem_limit_bytes=60 * 1024 * 1024
        ),
    )(date_slot, curve_store, taps, cash_amount[0].T, default_weight)
    return pl.pallas_call(
        split_kernel,
        out_shape=(
            jax.ShapeDtypeStruct((DATES, NSETS // 4), F32),
            jax.ShapeDtypeStruct((1, DATES, NODES), F32),
        ),
        in_specs=[whole],
        out_specs=(whole, whole),
    )(sums)


def solution(mesh):
    in_specs = (
        P("ccy", "path", None, None),
        P("ccy", None, None),
        P("ccy", None, None),
        P("ccy", None),
        P(),
        P(),
    )
    out_specs = (P(None, "ccy"), P("ccy", None, None))
    return jax.shard_map(local, mesh=mesh, in_specs=in_specs, out_specs=out_specs, check_vma=False)
```

```python
import jax
import jax.numpy as jnp
from jax import lax
from jax.experimental import pallas as pl
from jax.experimental.pallas import tpu as pltpu
from jax.sharding import PartitionSpec as P

NODES = 64
CFG = 1024
NSETS = 512
NCF = 16
TRADES = 2048
DATES = 16
HALF = DATES // 2
CHIP_PATHS = 128
ROWS = HALF * CHIP_PATHS
TOTAL_PATHS = 8192
SOFTEN = 0.04
LOG2E = 1.4426950408889634
CHUNK = 256
CHUNKS = CFG // CHUNK
TAPS = 24
MESH = pl.DeviceIdType.MESH
BF = jnp.bfloat16
F32 = jnp.float32
NT = (((1,), (1,)), ((), ()))
TN = (((0,), (0,)), ((), ()))


def coords():
    ccy = lax.axis_index("ccy")
    path = lax.axis_index("path")
    core = lax.rem(ccy, 2)
    z = lax.rem(path, 2) * 2 + lax.div(ccy, 2)
    x = lax.rem(lax.div(path, 2), 4)
    y = lax.div(path, 8)
    return y, x, z, core


def device(y, x, z, core):
    return (lax.rem(z, 2) * 2 + core, (y * 4 + x) * 2 + lax.div(z, 2))


def chip_index(y, x, z):
    return (y * 4 + x) * 4 + z


def shifted(i, y, x, z):
    b, c, a = lax.div(i, 16), lax.rem(lax.div(i, 4), 4), lax.rem(i, 4)
    return (
        lax.rem(y + a, 4),
        lax.rem(x + a + b, 4),
        lax.rem(z + a + c, 4),
    )


def remote(src, dst, send, recv, target):
    return pltpu.make_async_remote_copy(
        src_ref=src,
        dst_ref=dst,
        send_sem=send,
        recv_sem=recv,
        device_id=target,
        device_id_type=MESH,
    )


def aligned(start, size):
    if isinstance(start, int):
        return pl.ds(start, size)
    return pl.ds(pl.multiple_of(start, size), size)


def grid_tables(date, nodes):
    steps = lax.broadcasted_iota(jnp.int32, (1, CFG), 1) + 1 - 16 * (date + 1)
    steps = steps.astype(F32)
    place = jnp.clip(steps * (1.0 / 16.0), 1.0, float(NODES))
    node = (lax.broadcasted_iota(jnp.int32, (nodes, CFG), 0) + 1).astype(F32)
    weights = jnp.maximum(0.0, 1.0 - jnp.abs(place - node))
    return steps, steps * (1.0 / 32.0), weights


def prepare_trades(raw_i, raw_a, j, merged, onehot):
    amounts = raw_a[j]
    indices = raw_i[j, pl.ds(0, NCF), :]
    sums = jnp.zeros_like(amounts)
    for k in range(NCF):
        sums = sums + jnp.where(indices == indices[k : k + 1], amounts[k : k + 1], 0.0)
    merged[j] = sums
    sets = raw_i[j, pl.ds(NCF, 1), :]
    for s in range(0, NSETS, 64):
        ids = lax.broadcasted_iota(jnp.int32, (64, TRADES), 0) + s
        onehot[j, pl.ds(s, 64), :] = jnp.where(ids == sets, 1.0, 0.0).astype(BF)


def spread(raw_i, merged, j, base, start, flows):
    cols = pl.ds(start, 128)
    for part in range(0, CHUNK, 128):
        ids = [lax.broadcasted_iota(jnp.int32, (8, 128), 0) + (base + part + 8 * r) for r in range(16)]
        accs = [jnp.zeros((8, 128), F32)] * 16
        for k in range(NCF):
            where = jnp.broadcast_to(raw_i[j, pl.ds(k, 1), cols], (8, 128))
            worth = jnp.broadcast_to(merged[j, pl.ds(k, 1), cols], (8, 128))
            accs = [jnp.where(i == where, worth, acc) for i, acc in zip(ids, accs)]
        for r in range(0, 16, 2):
            total = jnp.concatenate(accs[r : r + 2], axis=0)
            high = total.astype(BF)
            flows[pl.ds(part + 8 * r, 16), cols] = high
            flows[pl.ds(CHUNK + part + 8 * r, 16), cols] = (total - high.astype(F32)).astype(BF)


def store_weights(core, mesh_w):
    for k in range(HALF):
        mesh_w[k] = grid_tables(core * HALF + k, NODES)[2].astype(BF)


def discounts(core, curves, h, discount, mesh_w):
    c = lax.rem(core + h, 2)
    for k in range(HALF):
        steps, remain, _ = grid_tables(core * HALF + k, 8)
        down = remain * -LOG2E
        live = steps[:, :256] > 0.0
        rows = pl.ds(k * CHIP_PATHS, CHIP_PATHS)
        for low_z in range(2):
            rate = lax.dot_general(curves[c, low_z, k], mesh_w[k], TN, preferred_element_type=F32)
            held = jnp.exp2(rate * down)
            first = (h * 2 + low_z) * CFG
            discount[rows, aligned(first, 256)] = jnp.where(live, held[:, :256], 0.0).astype(BF)
            discount[rows, pl.ds(first + 256, CFG - 256)] = held[:, 256:].astype(BF)


def price(core, tables, weight_ref, part, discount, value, slope, pull, mesh_w):
    def slopes(k, carry):
        rows = aligned(k * CHIP_PATHS, CHIP_PATHS)
        v = value[rows, :]
        square = v * v + SOFTEN
        inverse = lax.rsqrt(square)
        mean = jnp.sum(0.5 * (v + square * inverse), axis=0, keepdims=True) * (1.0 / TOTAL_PATHS)
        scale = weight_ref[pl.ds(core * HALF + k, 1), :] * (0.5 / TOTAL_PATHS)
        slope[rows, :] = (scale * (1.0 + v * inverse)).astype(BF)
        for i in range(4):
            part[i // 2, i % 2, pl.ds(k, 1), :] = mean[:, i * 128 : (i + 1) * 128]
        return carry

    lax.fori_loop(0, HALF, slopes, 0, unroll=2)

    def pull_group(n, carry):
        i, c = lax.div(n, 2), lax.rem(n, 2)
        cash = tables[lax.rem(core + lax.div(n, 4), 2), aligned(lax.rem(n, 4) * 512, 512), :]
        back = lax.dot_general(slope[...], cash, NT, preferred_element_type=F32)
        weighed = back * discount[:, aligned(n * 512, 512)].astype(F32)
        sums = weighed.reshape(HALF, CHIP_PATHS, 512).sum(axis=1)
        for k in range(HALF):
            pull[k, pl.ds(i, 1), aligned(c * 512, 512)] = sums[k : k + 1]
        return carry

    lax.fori_loop(0, 8, pull_group, 0, unroll=4)

    for k in range(HALF):
        _, remain, _ = grid_tables(core * HALF + k, 8)
        rest = pull[k] * (remain * -1.0)
        pieces = []
        for _ in range(3):
            piece = rest.astype(BF).astype(F32)
            rest = rest - piece
            pieces.append(piece)
        pieces.append(jnp.zeros_like(rest))
        stack = jnp.concatenate(pieces, axis=0).astype(BF)
        sums = lax.dot_general(stack, mesh_w[k], NT, preferred_element_type=F32)
        total = sums[:8] + sums[8:16] + sums[16:24]
        for i in range(4):
            part[i % 2, lax.rem(core + i // 2, 2), pl.ds(HALF + k, 1), pl.ds(0, NODES)] = total[i : i + 1]


def kernel(
    slot_ref, store, taps, amounts, weight_ref,
    out,
    got, curves, give, raw_i, raw_a, merged, onehot, flows, tables,
    discount, value, slope, pull, mesh_w, part, z_buf, y_buf, x_buf,
    a_send, a_recv, own_sem, l_sem, r_send, r_recv, p_send, p_recv, c_send, c_recv,
    z_send, z_recv, y_send, y_recv, x_send, x_recv,
):
    y, x, z, core = coords()
    low = lax.rem(z, 2)
    partner = device(y, x, z, 1 - core)
    up = device(y, x, lax.rem(z + 1, 4), core)
    down = device(y, x, lax.rem(z + 3, 4), core)
    me = chip_index(y, x, z)
    in_z = [lax.rem(z + i, 4) for i in range(1, 4)]
    in_y = [lax.rem(y + i, 4) for i in range(1, 4)]
    in_x = [lax.rem(x + i, 4) for i in range(1, 4)]

    barrier = pltpu.get_barrier_semaphore()

    def greet(i, carry):
        pl.semaphore_signal(
            barrier, inc=1, device_id=device(*shifted(i, y, x, z), core), device_id_type=MESH
        )
        return carry

    pl.semaphore_signal(barrier, inc=1, device_id=partner, device_id_type=MESH)
    for t in in_x:
        pl.semaphore_signal(barrier, inc=1, device_id=device(y, t, z, 1 - core), device_id_type=MESH)
    lax.fori_loop(1, 64, greet, 0)
    own_raw = [
        pltpu.make_async_copy(taps, raw_i.at[0], l_sem.at[0]),
        pltpu.make_async_copy(amounts, raw_a.at[0], l_sem.at[1]),
    ]
    for copy in own_raw:
        copy.start()
    for copy in own_raw:
        copy.wait()
    prepare_trades(raw_i, raw_a, 0, merged, onehot)

    halves = [pl.ds(0, TRADES // 2), pl.ds(TRADES // 2, TRADES // 2)]
    raw = []
    for h, target in enumerate((up, down)):
        raw.append(remote(taps.at[:, halves[h]], raw_i.at[1, :, halves[h]], r_send.at[2 * h], r_recv.at[2 * h], target))
        raw.append(
            remote(amounts.at[:, halves[h]], raw_a.at[1, :, halves[h]], r_send.at[2 * h + 1], r_recv.at[2 * h + 1], target)
        )

    def lanes(chip):
        return aligned(chip * CHIP_PATHS, CHIP_PATHS)

    def curve_copy(i):
        ty, tx, tz = shifted(i, y, x, z)
        return remote(
            store.at[0, :, :, lanes(chip_index(ty, tx, tz))],
            got.at[me],
            a_send.at[i],
            a_recv.at[me],
            device(ty, tx, tz, core),
        )

    def launch(i, carry):
        curve_copy(i).start()
        return carry

    own_copy = pltpu.make_async_copy(store.at[0, :, :, lanes(me)], got.at[me], own_sem)
    own_copy.start()

    def table_rows(n):
        return aligned(lax.rem(low + lax.div(n, CHUNKS), 2) * CFG + lax.rem(n, CHUNKS) * CHUNK, CHUNK)

    def table_copy(n, c):
        block = tables.at[c, table_rows(n), :]
        return remote(block, block, p_send.at[n], p_recv.at[n], partner)

    def build(n, carry):
        @pl.when(n == 1)
        def _():
            pl.semaphore_wait(barrier, 67)
            for copy in raw:
                copy.start()
            table_copy(jnp.int32(0), core).start()

        @pl.when(n == 2)
        def _():
            lax.fori_loop(1, 64, launch, 0)

        @pl.when(n == CHUNKS)
        def _():
            for copy in raw:
                copy.wait()
            prepare_trades(raw_i, raw_a, 1, merged, onehot)

        j, q = lax.div(n, CHUNKS), lax.rem(n, CHUNKS)
        for t in range(0, TRADES, 128):
            spread(raw_i, merged, j, q * CHUNK, t, flows)
        both = lax.dot_general(flows[...], onehot[j], NT, preferred_element_type=F32)
        tables[core, table_rows(n), :] = (both[:CHUNK] + both[CHUNK:]).astype(BF)

        @pl.when(n > 0)
        def _():
            table_copy(n, core).start()

        return carry

    lax.fori_loop(0, 2 * CHUNKS, build, 0)

    def landed(i, carry):
        curve_copy(i).wait_send()
        ty, tx, tz = shifted(i, y, x, z)
        source = chip_index(ty, tx, tz)
        remote(
            store.at[0, :, :, lanes(me)], got.at[source], a_send.at[i], a_recv.at[source],
            device(ty, tx, tz, core),
        ).wait_recv()
        return carry

    store_weights(core, mesh_w)
    for k in range(HALF):
        pull[k] = jnp.zeros((8, CFG), F32)
    part[...] = jnp.zeros_like(part)
    own_copy.wait()
    lax.fori_loop(1, 64, landed, 0)

    def pick(date, low_z):
        slot = slot_ref[date]
        place = lax.div(slot, 2)
        return got[lax.div(place, 2) * 4 + lax.rem(place, 2) * 2 + low_z, lax.rem(slot, 2)]

    for k in range(HALF):
        for low_z in range(2):
            give[low_z, k] = pick((1 - core) * HALF + k, low_z)
    trade = remote(give, curves.at[core], c_send, c_recv, partner)
    trade.start()
    for k in range(HALF):
        for low_z in range(2):
            curves[core, low_z, k] = pick(core * HALF + k, low_z)
    discounts(core, curves, 0, discount, mesh_w)
    trade.wait_send()
    remote(give, curves.at[1 - core], c_send, c_recv, partner).wait_recv()
    value[...] = jnp.dot(discount[:, pl.ds(0, 2 * CFG)], tables[core], preferred_element_type=F32)
    discounts(core, curves, 1, discount, mesh_w)
    for n in range(2 * CHUNKS):
        table_copy(jnp.int32(n), core).wait_send()
        table_copy(jnp.int32(n), 1 - core).wait_recv()
    value[...] += jnp.dot(discount[:, pl.ds(2 * CFG, 2 * CFG)], tables[1 - core], preferred_element_type=F32)

    price(core, tables, weight_ref, part, discount, value, slope, pull, mesh_w)

    def stage(source_of, buf, send, recv, here, others, device_of):
        sends = []
        for i, t in enumerate(others):
            copy = remote(source_of(t), buf.at[here], send.at[i], recv.at[here], device_of(t))
            copy.start()
            sends.append(copy)
        for i, t in enumerate(others):
            sends[i].wait_send()
            remote(source_of(here), buf.at[t], send.at[i], recv.at[t], device_of(t)).wait_recv()

    z_buf[z] = part[low]
    stage(
        lambda t: part.at[lax.rem(t, 2)], z_buf, z_send, z_recv, z, in_z,
        lambda t: device(y, x, t, core),
    )
    y_buf[y] = (z_buf[0] + z_buf[1]) + (z_buf[2] + z_buf[3])
    stage(lambda t: y_buf.at[y], y_buf, y_send, y_recv, y, in_y, lambda t: device(t, x, z, core))
    both = (y_buf[0] + y_buf[1]) + (y_buf[2] + y_buf[3])
    give_x = z_buf.at[0]
    give_x[...] = both
    sends = []
    for i, t in enumerate([x] + in_x):
        for c in range(2):
            if i == 0 and c == 0:
                continue
            to_core = lax.rem(core + c, 2)
            copy = remote(
                give_x.at[to_core], x_buf.at[core, x], x_send.at[2 * i + c], x_recv.at[core, x],
                device(y, t, z, to_core),
            )
            copy.start()
            sends.append((copy, t, to_core, 2 * i + c))
    x_buf[core, x] = give_x[core]
    for copy, t, from_core, n in sends:
        copy.wait_send()
        remote(
            give_x.at[core], x_buf.at[from_core, t], x_send.at[n], x_recv.at[from_core, t],
            device(y, t, z, from_core),
        ).wait_recv()
    for half in range(2):
        out[half] = (x_buf[half, 0] + x_buf[half, 1]) + (x_buf[half, 2] + x_buf[half, 3])


def split_kernel(sums, exposure, sens):
    for half in range(2):
        exposure[pl.ds(half * HALF, HALF), :] = sums[half, :HALF]
        sens[0, pl.ds(half * HALF, HALF), :] = sums[half, HALF:, :NODES]


def local(curve_store, cash_index, cash_amount, trade_set, date_slot, default_weight):
    taps = jnp.concatenate(
        [cash_index[0].T, trade_set, jnp.zeros((TAPS - NCF - 1, TRADES), jnp.int32)], axis=0
    )
    whole = pl.BlockSpec(memory_space=pltpu.VMEM)
    there = pl.BlockSpec(memory_space=pl.ANY)
    dma = pltpu.SemaphoreType.DMA
    quarter = (2 * HALF, 128)
    sums = pl.pallas_call(
        kernel,
        out_shape=jax.ShapeDtypeStruct((2, *quarter), F32),
        in_specs=[pl.BlockSpec(memory_space=pltpu.SMEM), there, there, there, whole],
        out_specs=whole,
        scratch_shapes=[
            pltpu.VMEM((64, 2, NODES, CHIP_PATHS), BF),
            pltpu.VMEM((2, 2, HALF, NODES, CHIP_PATHS), BF),
            pltpu.VMEM((2, HALF, NODES, CHIP_PATHS), BF),
            pltpu.VMEM((2, TAPS, TRADES), jnp.int32),
            pltpu.VMEM((2, NCF, TRADES), F32),
            pltpu.VMEM((2, NCF, TRADES), F32),
            pltpu.VMEM((2, NSETS, TRADES), BF),
            pltpu.VMEM((2 * CHUNK, TRADES), BF),
            pltpu.VMEM((2, 2 * CFG, NSETS), BF),
            pltpu.VMEM((ROWS, 4 * CFG), BF),
            pltpu.VMEM((ROWS, NSETS), F32),
            pltpu.VMEM((ROWS, NSETS), BF),
            pltpu.VMEM((HALF, 8, CFG), F32),
            pltpu.VMEM((HALF, NODES, CFG), BF),
            pltpu.VMEM((2, 2, *quarter), F32),
            pltpu.VMEM((4, 2, *quarter), F32),
            pltpu.VMEM((4, 2, *quarter), F32),
            pltpu.VMEM((2, 4, *quarter), F32),
            dma((64,)),
            dma((64,)),
            dma,
            dma((2,)),
            dma((4,)),
            dma((4,)),
            dma((2 * CHUNKS,)),
            dma((2 * CHUNKS,)),
            dma,
            dma,
            dma((3,)),
            dma((4,)),
            dma((3,)),
            dma((4,)),
            dma((8,)),
            dma((2, 4)),
        ],
        compiler_params=pltpu.CompilerParams(
            collective_id=0, has_side_effects=True, vmem_limit_bytes=60 * 1024 * 1024
        ),
    )(date_slot, curve_store, taps, cash_amount[0].T, default_weight)
    return pl.pallas_call(
        split_kernel,
        out_shape=(
            jax.ShapeDtypeStruct((DATES, NSETS // 4), F32),
            jax.ShapeDtypeStruct((1, DATES, NODES), F32),
        ),
        in_specs=[whole],
        out_specs=(whole, whole),
    )(sums)


def solution(mesh):
    in_specs = (
        P("ccy", "path", None, None),
        P("ccy", None, None),
        P("ccy", None, None),
        P("ccy", None),
        P(),
        P(),
    )
    out_specs = (P(None, "ccy"), P("ccy", None, None))
    return jax.shard_map(local, mesh=mesh, in_specs=in_specs, out_specs=out_specs, check_vma=False)
```

```python
import jax
import jax.numpy as jnp
from jax import lax
from jax.experimental import pallas as pl
from jax.experimental.pallas import tpu as pltpu
from jax.sharding import PartitionSpec as P

NODES = 64
CFG = 1024
NSETS = 512
NCF = 16
TRADES = 2048
DATES = 16
HALF = DATES // 2
CHIP_PATHS = 128
ROWS = HALF * CHIP_PATHS
TOTAL_PATHS = 8192
SOFTEN = 0.04
LOG2E = 1.4426950408889634
CHUNK = 256
CHUNKS = CFG // CHUNK
MESH = pl.DeviceIdType.MESH
BF = jnp.bfloat16
F32 = jnp.float32
NT = (((1,), (1,)), ((), ()))
TN = (((0,), (0,)), ((), ()))


def coords():
    ccy = lax.axis_index("ccy")
    path = lax.axis_index("path")
    core = lax.rem(ccy, 2)
    z = lax.rem(path, 2) * 2 + lax.div(ccy, 2)
    x = lax.rem(lax.div(path, 2), 4)
    y = lax.div(path, 8)
    return y, x, z, core


def device(y, x, z, core):
    return (lax.rem(z, 2) * 2 + core, (y * 4 + x) * 2 + lax.div(z, 2))


def chip_index(y, x, z):
    return (y * 4 + x) * 4 + z


def shifted(i, y, x, z):
    b, c, a = lax.div(i, 16), lax.rem(lax.div(i, 4), 4), lax.rem(i, 4)
    return (
        lax.rem(y + a, 4),
        lax.rem(x + a + b, 4),
        lax.rem(z + a + c, 4),
    )


def remote(src, dst, send, recv, target):
    return pltpu.make_async_remote_copy(
        src_ref=src,
        dst_ref=dst,
        send_sem=send,
        recv_sem=recv,
        device_id=target,
        device_id_type=MESH,
    )


def aligned(start, size):
    if isinstance(start, int):
        return pl.ds(start, size)
    return pl.ds(pl.multiple_of(start, size), size)


def grid_tables(date, nodes):
    steps = lax.broadcasted_iota(jnp.int32, (1, CFG), 1) + 1 - 16 * (date + 1)
    steps = steps.astype(F32)
    place = jnp.clip(steps * (1.0 / 16.0), 1.0, float(NODES))
    node = (lax.broadcasted_iota(jnp.int32, (nodes, CFG), 0) + 1).astype(F32)
    weights = jnp.maximum(0.0, 1.0 - jnp.abs(place - node))
    return steps, steps * (1.0 / 32.0), weights


def prepare_trades(raw_i, raw_a, raw_s, j, merged, onehot):
    amounts = raw_a[j]
    indices = raw_i[j]
    sums = jnp.zeros_like(amounts)
    for k in range(NCF):
        sums = sums + jnp.where(indices == indices[k : k + 1], amounts[k : k + 1], 0.0)
    merged[j] = sums
    sets = raw_s[j]
    for s in range(0, NSETS, 64):
        ids = lax.broadcasted_iota(jnp.int32, (64, TRADES), 0) + s
        onehot[j, pl.ds(s, 64), :] = jnp.where(ids == sets, 1.0, 0.0).astype(BF)


def spread(raw_i, merged, j, base, start, flows):
    cols = pl.ds(start, 128)
    for part in range(0, CHUNK, 128):
        ids = [lax.broadcasted_iota(jnp.int32, (8, 128), 0) + (base + part + 8 * r) for r in range(16)]
        accs = [jnp.zeros((8, 128), F32)] * 16
        for k in range(NCF):
            where = jnp.broadcast_to(raw_i[j, pl.ds(k, 1), cols], (8, 128))
            worth = jnp.broadcast_to(merged[j, pl.ds(k, 1), cols], (8, 128))
            accs = [jnp.where(i == where, worth, acc) for i, acc in zip(ids, accs)]
        for r in range(0, 16, 2):
            total = jnp.concatenate(accs[r : r + 2], axis=0)
            high = total.astype(BF)
            flows[pl.ds(part + 8 * r, 16), cols] = high
            flows[pl.ds(CHUNK + part + 8 * r, 16), cols] = (total - high.astype(F32)).astype(BF)


def store_weights(core, mesh_w):
    for k in range(HALF):
        mesh_w[k] = grid_tables(core * HALF + k, NODES)[2].astype(BF)


def discounts(core, curves, h, discount, mesh_w):
    c = lax.rem(core + h, 2)
    for k in range(HALF):
        steps, remain, _ = grid_tables(core * HALF + k, 8)
        down = remain * -LOG2E
        live = steps[:, :256] > 0.0
        rows = pl.ds(k * CHIP_PATHS, CHIP_PATHS)
        for low_z in range(2):
            rate = lax.dot_general(curves[c, low_z, k], mesh_w[k], TN, preferred_element_type=F32)
            held = jnp.exp2(rate * down)
            first = (h * 2 + low_z) * CFG
            discount[rows, aligned(first, 256)] = jnp.where(live, held[:, :256], 0.0).astype(BF)
            discount[rows, pl.ds(first + 256, CFG - 256)] = held[:, 256:].astype(BF)


def price(core, tables, weight_ref, part, discount, value, slope, pull, mesh_w):
    def slopes(k, carry):
        rows = aligned(k * CHIP_PATHS, CHIP_PATHS)
        v = value[rows, :]
        square = v * v + SOFTEN
        inverse = lax.rsqrt(square)
        mean = jnp.sum(0.5 * (v + square * inverse), axis=0, keepdims=True) * (1.0 / TOTAL_PATHS)
        scale = weight_ref[pl.ds(core * HALF + k, 1), :] * (0.5 / TOTAL_PATHS)
        slope[rows, :] = (scale * (1.0 + v * inverse)).astype(BF)
        for i in range(4):
            part[i // 2, i % 2, pl.ds(k, 1), :] = mean[:, i * 128 : (i + 1) * 128]
        return carry

    lax.fori_loop(0, HALF, slopes, 0, unroll=2)

    def pull_group(n, carry):
        i, c = lax.div(n, 2), lax.rem(n, 2)
        cash = tables[lax.rem(core + lax.div(n, 4), 2), aligned(lax.rem(n, 4) * 512, 512), :]
        back = lax.dot_general(slope[...], cash, NT, preferred_element_type=F32)
        weighed = back * discount[:, aligned(n * 512, 512)].astype(F32)
        sums = weighed.reshape(HALF, CHIP_PATHS, 512).sum(axis=1)
        for k in range(HALF):
            pull[k, pl.ds(i, 1), aligned(c * 512, 512)] = sums[k : k + 1]
        return carry

    lax.fori_loop(0, 8, pull_group, 0, unroll=4)

    for k in range(HALF):
        _, remain, _ = grid_tables(core * HALF + k, 8)
        rest = pull[k] * (remain * -1.0)
        pieces = []
        for _ in range(3):
            piece = rest.astype(BF).astype(F32)
            rest = rest - piece
            pieces.append(piece)
        pieces.append(jnp.zeros_like(rest))
        stack = jnp.concatenate(pieces, axis=0).astype(BF)
        sums = lax.dot_general(stack, mesh_w[k], NT, preferred_element_type=F32)
        total = sums[:8] + sums[8:16] + sums[16:24]
        for i in range(4):
            part[i % 2, lax.rem(core + i // 2, 2), pl.ds(HALF + k, 1), pl.ds(0, NODES)] = total[i : i + 1]


def kernel(
    slot_ref, store, taps, amounts, sets, weight_ref,
    out,
    got, curves, give, raw_i, raw_a, raw_s, merged, onehot, flows, tables,
    discount, value, slope, pull, mesh_w, part, z_buf, y_buf, x_buf,
    a_send, a_recv, own_sem, l_sem, r_send, r_recv, p_send, p_recv, c_send, c_recv,
    z_send, z_recv, y_send, y_recv, x_send, x_recv,
):
    y, x, z, core = coords()
    low = lax.rem(z, 2)
    partner = device(y, x, z, 1 - core)
    up = device(y, x, lax.rem(z + 1, 4), core)
    down = device(y, x, lax.rem(z + 3, 4), core)
    me = chip_index(y, x, z)
    in_z = [lax.rem(z + i, 4) for i in range(1, 4)]
    in_y = [lax.rem(y + i, 4) for i in range(1, 4)]
    in_x = [lax.rem(x + i, 4) for i in range(1, 4)]

    barrier = pltpu.get_barrier_semaphore()

    def greet(i, carry):
        pl.semaphore_signal(
            barrier, inc=1, device_id=device(*shifted(i, y, x, z), core), device_id_type=MESH
        )
        return carry

    pl.semaphore_signal(barrier, inc=1, device_id=partner, device_id_type=MESH)
    for t in in_x:
        pl.semaphore_signal(barrier, inc=1, device_id=device(y, t, z, 1 - core), device_id_type=MESH)
    lax.fori_loop(1, 64, greet, 0)
    own_raw = [
        pltpu.make_async_copy(taps, raw_i.at[0], l_sem.at[0]),
        pltpu.make_async_copy(amounts, raw_a.at[0], l_sem.at[1]),
        pltpu.make_async_copy(sets, raw_s.at[0], l_sem.at[2]),
    ]
    for copy in own_raw:
        copy.start()
    for copy in own_raw:
        copy.wait()
    prepare_trades(raw_i, raw_a, raw_s, 0, merged, onehot)

    halves = [pl.ds(0, TRADES // 2), pl.ds(TRADES // 2, TRADES // 2)]
    raw = []
    for h, target in enumerate((up, down)):
        for i, (mine, there) in enumerate(((taps, raw_i), (amounts, raw_a), (sets, raw_s))):
            raw.append(
                remote(
                    mine.at[:, halves[h]], there.at[1, :, halves[h]], r_send.at[3 * h + i], r_recv.at[3 * h + i], target
                )
            )

    def lanes(chip):
        return aligned(chip * CHIP_PATHS, CHIP_PATHS)

    def curve_copy(i):
        ty, tx, tz = shifted(i, y, x, z)
        return remote(
            store.at[0, :, :, lanes(chip_index(ty, tx, tz))],
            got.at[me],
            a_send.at[i],
            a_recv.at[me],
            device(ty, tx, tz, core),
        )

    def launch(i, carry):
        curve_copy(i).start()
        return carry

    own_copy = pltpu.make_async_copy(store.at[0, :, :, lanes(me)], got.at[me], own_sem)
    own_copy.start()

    def table_rows(n):
        return aligned(lax.rem(low + lax.div(n, CHUNKS), 2) * CFG + lax.rem(n, CHUNKS) * CHUNK, CHUNK)

    def table_copy(n, c):
        block = tables.at[c, table_rows(n), :]
        return remote(block, block, p_send.at[n], p_recv.at[n], partner)

    def build(n, carry):
        @pl.when(n == 1)
        def _():
            pl.semaphore_wait(barrier, 67)
            for copy in raw:
                copy.start()
            table_copy(jnp.int32(0), core).start()

        @pl.when(n == 2)
        def _():
            lax.fori_loop(1, 64, launch, 0)

        @pl.when(n == CHUNKS)
        def _():
            for copy in raw:
                copy.wait()
            prepare_trades(raw_i, raw_a, raw_s, 1, merged, onehot)

        j, q = lax.div(n, CHUNKS), lax.rem(n, CHUNKS)
        for t in range(0, TRADES, 128):
            spread(raw_i, merged, j, q * CHUNK, t, flows)
        both = lax.dot_general(flows[...], onehot[j], NT, preferred_element_type=F32)
        tables[core, table_rows(n), :] = (both[:CHUNK] + both[CHUNK:]).astype(BF)

        @pl.when(n > 0)
        def _():
            table_copy(n, core).start()

        return carry

    lax.fori_loop(0, 2 * CHUNKS, build, 0)

    def landed(i, carry):
        curve_copy(i).wait_send()
        ty, tx, tz = shifted(i, y, x, z)
        source = chip_index(ty, tx, tz)
        remote(
            store.at[0, :, :, lanes(me)], got.at[source], a_send.at[i], a_recv.at[source],
            device(ty, tx, tz, core),
        ).wait_recv()
        return carry

    store_weights(core, mesh_w)
    for k in range(HALF):
        pull[k] = jnp.zeros((8, CFG), F32)
    part[...] = jnp.zeros_like(part)
    own_copy.wait()
    lax.fori_loop(1, 64, landed, 0)

    def pick(date, low_z):
        slot = slot_ref[date]
        place = lax.div(slot, 2)
        return got[lax.div(place, 2) * 4 + lax.rem(place, 2) * 2 + low_z, lax.rem(slot, 2)]

    for k in range(HALF):
        for low_z in range(2):
            give[low_z, k] = pick((1 - core) * HALF + k, low_z)
    trade = remote(give, curves.at[core], c_send, c_recv, partner)
    trade.start()
    for k in range(HALF):
        for low_z in range(2):
            curves[core, low_z, k] = pick(core * HALF + k, low_z)
    discounts(core, curves, 0, discount, mesh_w)
    trade.wait_send()
    remote(give, curves.at[1 - core], c_send, c_recv, partner).wait_recv()
    value[...] = jnp.dot(discount[:, pl.ds(0, 2 * CFG)], tables[core], preferred_element_type=F32)
    discounts(core, curves, 1, discount, mesh_w)
    for n in range(2 * CHUNKS):
        table_copy(jnp.int32(n), core).wait_send()
        table_copy(jnp.int32(n), 1 - core).wait_recv()
    value[...] += jnp.dot(discount[:, pl.ds(2 * CFG, 2 * CFG)], tables[1 - core], preferred_element_type=F32)

    price(core, tables, weight_ref, part, discount, value, slope, pull, mesh_w)

    def stage(source_of, buf, send, recv, here, others, device_of):
        sends = []
        for i, t in enumerate(others):
            copy = remote(source_of(t), buf.at[here], send.at[i], recv.at[here], device_of(t))
            copy.start()
            sends.append(copy)
        for i, t in enumerate(others):
            sends[i].wait_send()
            remote(source_of(here), buf.at[t], send.at[i], recv.at[t], device_of(t)).wait_recv()

    z_buf[z] = part[low]
    stage(
        lambda t: part.at[lax.rem(t, 2)], z_buf, z_send, z_recv, z, in_z,
        lambda t: device(y, x, t, core),
    )
    y_buf[y] = (z_buf[0] + z_buf[1]) + (z_buf[2] + z_buf[3])
    stage(lambda t: y_buf.at[y], y_buf, y_send, y_recv, y, in_y, lambda t: device(t, x, z, core))
    both = (y_buf[0] + y_buf[1]) + (y_buf[2] + y_buf[3])
    give_x = z_buf.at[0]
    give_x[...] = both
    sends = []
    for i, t in enumerate([x] + in_x):
        for c in range(2):
            if i == 0 and c == 0:
                continue
            to_core = lax.rem(core + c, 2)
            copy = remote(
                give_x.at[to_core], x_buf.at[core, x], x_send.at[2 * i + c], x_recv.at[core, x],
                device(y, t, z, to_core),
            )
            copy.start()
            sends.append((copy, t, to_core, 2 * i + c))
    x_buf[core, x] = give_x[core]
    for copy, t, from_core, n in sends:
        copy.wait_send()
        remote(
            give_x.at[core], x_buf.at[from_core, t], x_send.at[n], x_recv.at[from_core, t],
            device(y, t, z, from_core),
        ).wait_recv()
    for half in range(2):
        out[half] = (x_buf[half, 0] + x_buf[half, 1]) + (x_buf[half, 2] + x_buf[half, 3])


def split_kernel(sums, exposure, sens):
    for half in range(2):
        exposure[pl.ds(half * HALF, HALF), :] = sums[half, :HALF]
        sens[0, pl.ds(half * HALF, HALF), :] = sums[half, HALF:, :NODES]


def local(curve_store, cash_index, cash_amount, trade_set, date_slot, default_weight):
    whole = pl.BlockSpec(memory_space=pltpu.VMEM)
    there = pl.BlockSpec(memory_space=pl.ANY)
    dma = pltpu.SemaphoreType.DMA
    quarter = (2 * HALF, 128)
    sums = pl.pallas_call(
        kernel,
        out_shape=jax.ShapeDtypeStruct((2, *quarter), F32),
        in_specs=[pl.BlockSpec(memory_space=pltpu.SMEM), there, there, there, there, whole],
        out_specs=whole,
        scratch_shapes=[
            pltpu.VMEM((64, 2, NODES, CHIP_PATHS), BF),
            pltpu.VMEM((2, 2, HALF, NODES, CHIP_PATHS), BF),
            pltpu.VMEM((2, HALF, NODES, CHIP_PATHS), BF),
            pltpu.VMEM((2, NCF, TRADES), jnp.int32),
            pltpu.VMEM((2, NCF, TRADES), F32),
            pltpu.VMEM((2, 1, TRADES), jnp.int32),
            pltpu.VMEM((2, NCF, TRADES), F32),
            pltpu.VMEM((2, NSETS, TRADES), BF),
            pltpu.VMEM((2 * CHUNK, TRADES), BF),
            pltpu.VMEM((2, 2 * CFG, NSETS), BF),
            pltpu.VMEM((ROWS, 4 * CFG), BF),
            pltpu.VMEM((ROWS, NSETS), F32),
            pltpu.VMEM((ROWS, NSETS), BF),
            pltpu.VMEM((HALF, 8, CFG), F32),
            pltpu.VMEM((HALF, NODES, CFG), BF),
            pltpu.VMEM((2, 2, *quarter), F32),
            pltpu.VMEM((4, 2, *quarter), F32),
            pltpu.VMEM((4, 2, *quarter), F32),
            pltpu.VMEM((2, 4, *quarter), F32),
            dma((64,)),
            dma((64,)),
            dma,
            dma((3,)),
            dma((6,)),
            dma((6,)),
            dma((2 * CHUNKS,)),
            dma((2 * CHUNKS,)),
            dma,
            dma,
            dma((3,)),
            dma((4,)),
            dma((3,)),
            dma((4,)),
            dma((8,)),
            dma((2, 4)),
        ],
        compiler_params=pltpu.CompilerParams(
            collective_id=0, has_side_effects=True, vmem_limit_bytes=60 * 1024 * 1024
        ),
    )(date_slot, curve_store, cash_index[0].T, cash_amount[0].T, trade_set, default_weight)
    return pl.pallas_call(
        split_kernel,
        out_shape=(
            jax.ShapeDtypeStruct((DATES, NSETS // 4), F32),
            jax.ShapeDtypeStruct((1, DATES, NODES), F32),
        ),
        in_specs=[whole],
        out_specs=(whole, whole),
    )(sums)


def solution(mesh):
    in_specs = (
        P("ccy", "path", None, None),
        P("ccy", None, None),
        P("ccy", None, None),
        P("ccy", None),
        P(),
        P(),
    )
    out_specs = (P(None, "ccy"), P("ccy", None, None))
    return jax.shard_map(local, mesh=mesh, in_specs=in_specs, out_specs=out_specs, check_vma=False)
```
